32 devices in a mesh: board: 16 (over z, y, x), hand: 2 (over core).
Axes of the slice: x: 2, y: 2, z: 4, core: 2. Of those that a mesh axis runs over, the one named last changes fastest.
Arguments:
- opp_reach: bfloat16 [1024, 1326], P('board', 'hand'), may hold values from 0.019897461 to 1
- hand_rank: int32 [1024, 1326], P('board'), may hold values from 0 to 1325, as said below
- hand_cards: int32 [1326, 2], replicated, may hold values from 0 to 51, as said below
- pot: float32 [1024], P('board'), may hold values from 1 to 12
- bet_frac: float32 [1024], P('board'), may hold values from 0.25 to 1.5
- trav_reach: float32 [1326], P('hand'), may hold values from 0.02 to 1
Outputs:
- board_values: float32 [1024, 1326], P('board', 'hand')
- hand_values: float32 [1326], P('hand')
- exploitability: float32 [], replicated
The draws below stay inside these ranges and needn't reach their ends.
Inputs may be any that keep to these rules, and one draw needn't show every extreme that they name: hand_rank[b, i] is the number of hands strictly weaker than hand i on board b; equal ranks tie. `hand_cards`: the rows are the 1326 distinct pairs of two different cards, smaller card first, in an order drawn from the seed.
All inputs are finite; a program needn't handle non-finite values.
Results may differ from the reference program's by a relative error of at most 0.0003.
Values may be sent and summed in bfloat16 or wider, within the bound.
A program may use at most 64 MiB of HBM per device.

```python
import math
import jax
import jax.numpy as jnp
import numpy as np
from jax import lax

CARDS = 52
H = 1326
BOARDS = 1024


def showdown_order(key):
    seeded = jax.random.fold_in(key, 7)
    hand_key, board_key = jax.random.split(seeded)
    strength = jax.random.randint(hand_key, (1, H), 0, 3 * H // 4)
    noise = jax.random.randint(board_key, (BOARDS, H), 0, H // 2)
    scores = (strength + noise).astype(jnp.int32)
    ordering = jnp.argsort(scores, axis=1, stable=True).astype(jnp.int32)
    ranked = jnp.take_along_axis(scores, ordering, axis=1)
    positions = lax.broadcasted_iota(jnp.int32, (BOARDS, H), 1)
    fresh = jnp.concatenate([jnp.ones((BOARDS, 1), jnp.bool_), ranked[:, 1:] != ranked[:, :-1]], axis=1)
    starts = lax.cummax(jnp.where(fresh, positions, 0), axis=1)
    board_rows = lax.broadcasted_iota(jnp.int32, (BOARDS, H), 0)
    rank_table = jnp.zeros((BOARDS, H), jnp.int32).at[board_rows, ordering].set(starts)
    return rank_table


def draw_hand_rank(key, part):
    return showdown_order(key)


def draw_hand_cards(key, part):
    lower_card, upper_card = np.triu_indices(CARDS, 1)
    pairs = jnp.stack([jnp.asarray(lower_card), jnp.asarray(upper_card)], axis=1).astype(jnp.int32)
    shuffle = jax.random.permutation(jax.random.fold_in(key, 11), H)
    return pairs[shuffle]


def draw_pot(key, part):
    seeded = jax.random.fold_in(key, 13)
    spread = jnp.arange(BOARDS, dtype=jnp.float32) / max(BOARDS - 1, 1)
    level = jnp.exp(jax.random.uniform(seeded, (BOARDS,), jnp.float32, 0.0, math.log(4.0)))
    return ((1.0 + 2.0 * spread) * level).astype(jnp.float32)


def shard_levels(stream_key, extent, pieces, low, top_value):
    level, own = 1.0, jax.random.fold_in(stream_key, 6)
    for position, parts in pieces:
        steps = jnp.exp(jax.random.uniform(jax.random.fold_in(own, position), (parts,), jnp.float32, low / len(pieces), top_value / len(pieces)))
        level = level * jnp.repeat(steps, extent[position] // parts).reshape([-1 if axis == position else 1 for axis in range(len(extent))])
    return level


def setup_inputs(seed: int = 0) -> dict:
    streams_of = jax.random.split(jax.random.key(seed), 7)
    return {
        "opp_reach": jnp.clip(jnp.exp(math.log(1.0) - 3.9171631 * jax.random.uniform(streams_of[0], (BOARDS, H), jnp.float32) ** shard_levels(streams_of[0], (BOARDS, H), ((0, 16), (1, 2)), -0.2, 0.2)), 0.019897461, 1.0).astype(jnp.bfloat16),
        "hand_rank": draw_hand_rank(jax.random.fold_in(streams_of[6], 71), 0),
        "hand_cards": draw_hand_cards(jax.random.fold_in(streams_of[6], 71), 0),
        "pot": draw_pot(jax.random.fold_in(streams_of[6], 71), 0),
        "bet_frac": jnp.clip(0.25 + 1.25 * jax.random.uniform(streams_of[4], (BOARDS,), jnp.float32) ** shard_levels(streams_of[4], (BOARDS,), ((0, 16),), -0.2, 0.2), 0.25, 1.5),
        "trav_reach": jnp.clip(jnp.exp(math.log(1.0) - 3.912023 * jax.random.uniform(streams_of[5], (H,), jnp.float32) ** shard_levels(streams_of[5], (H,), ((0, 2),), -0.2, 0.2)), 0.02, 1.0),
    }


def incidence(hand_cards):
    card_ids = jnp.arange(CARDS, dtype=jnp.int32)
    return ((hand_cards[:, 0:1] == card_ids) | (hand_cards[:, 1:2] == card_ids)).astype(jnp.float32)


def showdown(opp_reach, hand_rank, hand_cards):
    card_hold = incidence(hand_cards)
    first_card = hand_cards[:, 0]
    second_card = hand_cards[:, 1]
    positions = jnp.arange(H, dtype=jnp.int32)

    def one_board(board_data):
        rank_row, reach_row = board_data
        order_row = jnp.argsort(rank_row, stable=True).astype(jnp.int32)
        own_reach = reach_row.astype(jnp.float32)
        weighted = own_reach[:, None] * card_hold
        ordered = weighted[order_row]
        prefix = jnp.concatenate([jnp.zeros((1, CARDS), jnp.float32), jnp.cumsum(ordered, axis=0)], axis=0)
        share = jnp.sum(prefix, axis=1) * 0.5
        sorted_rank = rank_row[order_row]
        group_marks = jnp.where(sorted_rank == positions, positions, H)
        shifted = jnp.concatenate([group_marks[1:], jnp.full((1,), H, jnp.int32)])
        next_start = lax.cummin(shifted, axis=0, reverse=True)
        tie_end = next_start[rank_row]

        def blocked(row_index):
            return share[row_index] - prefix[row_index, first_card] - prefix[row_index, second_card]

        beaten = blocked(rank_row)
        reached = blocked(tie_end) + own_reach
        live_mass = blocked(jnp.full((H,), H, jnp.int32)) + own_reach
        return beaten + reached - live_mass, live_mass

    return lax.map(one_board, (hand_rank, opp_reach))


def reference(opp_reach, hand_rank, hand_cards, pot, bet_frac, trav_reach):
    margin, live_mass = showdown(opp_reach, hand_rank, hand_cards)
    half_pot = (0.5 * pot)[:, None]
    call_value = (half_pot + (bet_frac * pot)[:, None]) * margin / H
    fold_value = -half_pot * live_mass / H
    board_values = jnp.maximum(call_value, fold_value)
    hand_values = jnp.mean(board_values, axis=0)
    opp_mass = jnp.mean(half_pot * live_mass / H, axis=0)
    exploit = jnp.sum(trav_reach * hand_values) / jnp.sum(trav_reach * opp_mass)
    return board_values, hand_values, exploit
```

```python
import functools

import jax
import jax.numpy as jnp
from jax import lax
from jax.experimental import pallas as pl
from jax.experimental.pallas import tpu as pltpu
from jax.sharding import PartitionSpec as P

CARDS = 52
LANES = 128
STRIDE = 64
DIGIT = 32
MESH = pl.DeviceIdType.MESH
F32 = jnp.float32
BF16 = jnp.bfloat16
NT = (((1,), (1,)), ((), ()))


def up(n, m):
    return (n + m - 1) // m * m


def iota(shape, axis, dtype=jnp.int32):
    return lax.broadcasted_iota(jnp.int32, shape, axis).astype(dtype)


def column(row):
    n = row.shape[1]
    diag = iota((n, n), 0) == iota((n, n), 1)
    return jnp.sum(jnp.where(diag, row, 0.0), axis=1, keepdims=True)


def split2(x):
    top = x.astype(BF16)
    return top, (x - top.astype(F32)).astype(BF16)


def split3(x):
    top = x.astype(BF16)
    rest = x - top.astype(F32)
    mid, low = split2(rest)
    return top, mid, low


def lookup(table, at):
    return jnp.take_along_axis(table, at, axis=1, mode="promise_in_bounds")


def kernel(
    nb, opp, rank, cards, pot, bet, trav, bv_out, hv_out, ex_out,
    pt, key, rhi, rlo, wf, xs, got, tt, wt, st, eqs, c1, rt, gg, ct, mm, sb, msg, recva, recvb,
    s_reach, s_ct, s_m, send_a, recv_a, send_b, recv_b,
):
    me, h = lax.axis_index("board"), lax.axis_index("hand")
    boards, half = opp.shape
    hands = rank.shape[1]
    own = boards // 2
    hp = wf.shape[1]
    halfp = mm.shape[1]
    mine = pl.multiple_of(h * own, own)
    theirs = pl.multiple_of((1 - h) * own, own)
    partner = (me, 1 - h)
    pairs = CARDS // 2
    group = LANES // own
    blocks = tt.shape[0]
    left = h == 0

    barrier = pltpu.get_barrier_semaphore()
    for k in range(nb):
        peer = lax.rem(me + k, nb)
        if k:
            pl.semaphore_signal(barrier, inc=1, device_id=(peer, h), device_id_type=MESH)
        pl.semaphore_signal(barrier, inc=1, device_id=(peer, 1 - h), device_id_type=MESH)

    key[...] = jnp.full(key.shape, -1, jnp.int32)
    key[:, :hands] = cards[...]
    u, v = key[0:1, :], key[1:2, :]
    rows = rank[pl.ds(mine, own), :]
    rhi[...] = jnp.zeros(rhi.shape, F32)
    rlo[...] = jnp.zeros(rlo.shape, F32)
    rhi[:, :hands] = (rows // DIGIT).astype(F32)
    rlo[:, :hands] = (rows % DIGIT).astype(F32)

    depth = iota((STRIDE, hp), 0, F32).astype(BF16)

    def build(c, carry):
        other = jnp.where(u == c, v, jnp.where(v == c, u, -1)).astype(F32).astype(BF16)
        hit = depth == jnp.broadcast_to(other, (STRIDE, hp))
        start = pl.multiple_of(c * STRIDE, STRIDE)
        pt[pl.ds(start, STRIDE), :] = jnp.where(hit, jnp.ones((), BF16), jnp.zeros((), BF16))
        return carry

    lax.fori_loop(0, CARDS // 2, build, 0)

    pl.semaphore_wait(barrier, 2 * nb - 1)
    reach_copy = pltpu.make_async_remote_copy(
        src_ref=opp.at[pl.ds(theirs, own)], dst_ref=got, send_sem=s_reach.at[0], recv_sem=s_reach.at[1],
        device_id=partner, device_id_type=MESH,
    )
    reach_copy.start()
    lax.fori_loop(CARDS // 2, CARDS, build, 0)

    card_row = iota((LANES, hp), 0)
    hold = ((card_row == u) | (card_row == v)).astype(F32).astype(BF16)
    shift = hp - half
    u_r, v_r = pltpu.roll(key[...], shift, 1)[0:1, :halfp], pltpu.roll(key[...], shift, 1)[1:2, :halfp]
    u_m = jnp.where(left, u[:, :halfp], u_r)
    v_m = jnp.where(left, v[:, :halfp], v_r)

    nhi = c1.shape[2] // 2
    hi_row = iota((nhi, hp), 0, F32).astype(BF16)

    def digit(b, carry):
        hi_b = jnp.broadcast_to(rhi[pl.ds(b, 1), :].astype(BF16), (nhi, hp))
        eq = jnp.where(hi_row == hi_b, jnp.ones((), BF16), jnp.zeros((), BF16))
        eqs[b, 0:nhi, :] = eq
        eqs[b, nhi : 2 * nhi, :] = eq
        return carry

    lax.fori_loop(0, own, digit, 0, unroll=2)

    reach_copy.wait()
    here, there = opp[pl.ds(mine, own), :].astype(F32), got[...].astype(F32)
    wf[...] = jnp.zeros(wf.shape, F32)
    wf[:, :half] = jnp.where(left, there, here)
    second = pltpu.roll(wf[...], half, 1)
    wf[...] = jnp.zeros(wf.shape, F32)
    wf[:, :half] = jnp.where(left, here, there)
    w_all = wf[...] + second
    wf[...] = w_all
    w_low = w_all.astype(BF16)

    ct[pl.ds(mine, own), :] = lax.dot_general(w_low, hold, NT, preferred_element_type=F32)
    ct_copy = pltpu.make_async_remote_copy(
        src_ref=ct.at[pl.ds(mine, own)], dst_ref=ct.at[pl.ds(mine, own)], send_sem=s_ct.at[0], recv_sem=s_ct.at[1],
        device_id=partner, device_id_type=MESH,
    )
    ct_copy.start()

    xs[0:own, :] = rhi[...].astype(BF16)
    xs[own : 2 * own, :] = rlo[...].astype(BF16)
    xs[2 * own :, :] = w_low
    table = lax.dot_general(xs[...], pt[...], NT, preferred_element_type=F32)
    t_tab = table[0:own] * float(DIGIT) + table[own : 2 * own]
    w_tab = table[2 * own :]
    for blk in range(blocks):
        for src, dst in ((t_tab, tt), (w_tab, wt)):
            parts = []
            for q in range(group):
                p = blk * group + q
                if p < pairs:
                    parts.append(src[:, p * LANES : (p + 1) * LANES])
                else:
                    parts.append(jnp.zeros((own, LANES), F32))
            dst[blk] = jnp.concatenate(parts, axis=0).T

    used = up(CARDS, 8)
    st[...] = jnp.zeros(st.shape, F32)

    def correct(n, carry):
        blk, off = n // 2, pl.multiple_of((n % 2) * STRIDE, STRIDE)
        t_here = tt[blk, pl.ds(off, used), :]
        acc = jnp.zeros((used, LANES), F32)
        for e in range(CARDS):
            te = tt[blk, pl.ds(off + e, 1), :]
            we = wt[blk, pl.ds(off + e, 1), :]
            acc = acc + jnp.where(t_here > te, we, jnp.where(t_here < te, -we, 0.0))
        st[blk, pl.ds(off, used), :] = acc
        return carry

    lax.fori_loop(0, 2 * blocks, correct, 0)
    pieces = []
    for p in range(pairs):
        blk, q = p // group, p % group
        if q == 0:
            back = st[blk].T
        pieces.append(back[q * own : (q + 1) * own])
    s_tab = jnp.concatenate(pieces, axis=1)
    s_top, s_low = split2(s_tab)
    scattered = jnp.dot(jnp.concatenate([s_top, s_low], axis=0), pt[...], preferred_element_type=F32)
    corr = scattered[:own] + scattered[own:]

    nlo = c1.shape[1]
    lo_row = iota((nlo, hp), 0, F32).astype(BF16)

    def hist(b, carry):
        lo_b = jnp.broadcast_to(rlo[pl.ds(b, 1), :].astype(BF16), (nlo, hp))
        w_b = jnp.broadcast_to(wf[pl.ds(b, 1), :].astype(BF16), (nlo, hp))
        lw = jnp.where(lo_row > lo_b, w_b, jnp.where(lo_row < lo_b, -w_b, jnp.zeros((), BF16)))
        part = lax.dot_general(lw, eqs[b], NT, preferred_element_type=F32)
        c1[b] = part
        rt[pl.ds(b, 1), :] = part[DIGIT : DIGIT + 1, :]
        return carry

    lax.fori_loop(0, own, hist, 0, unroll=8)
    wide = 2 * nhi
    a, z = iota((wide, wide), 0), iota((wide, wide), 1)
    z = jnp.where(z >= nhi, z - nhi, z)
    sgn = jnp.where(a >= nhi, 0, jnp.where(z > a, 1, jnp.where(z < a, -1, 0))).astype(F32).astype(BF16)
    r0, r1, r2 = split3(rt[...])
    rt[...] = (
        jnp.dot(r0, sgn, preferred_element_type=F32)
        + jnp.dot(r1, sgn, preferred_element_type=F32)
        + jnp.dot(r2, sgn, preferred_element_type=F32)
    )
    lo_f = iota((DIGIT, hp), 0, F32)
    first = iota((DIGIT, wide), 1) < nhi

    def pick(b, carry):
        tab = c1[b, 0:DIGIT, :] + rt[pl.ds(b, 1), :]
        top = tab.astype(BF16).astype(F32)
        lhs = jnp.where(first, top, tab - top).astype(BF16)
        d = jnp.dot(lhs, eqs[b], preferred_element_type=F32)
        hit = lo_f == rlo[pl.ds(b, 1), :]
        gg[pl.ds(b, 1), :] = jnp.sum(jnp.where(hit, d, 0.0), axis=0, keepdims=True)
        return carry

    lax.fori_loop(0, own, pick, 0, unroll=8)
    margin = gg[...] - corr

    m_left = margin[:, :halfp]
    m_right = pltpu.roll(margin, shift, 1)[:, :halfp]
    sb[...] = jnp.where(left, m_right, m_left)
    m_copy = pltpu.make_async_remote_copy(
        src_ref=sb, dst_ref=mm.at[pl.ds(mine, own)], send_sem=s_m.at[0], recv_sem=s_m.at[1],
        device_id=partner, device_id_type=MESH,
    )
    m_copy.start()
    mm[pl.ds(mine, own), :] = jnp.where(left, m_left, m_right)

    ct_copy.wait()
    totals = ct[...]
    taken_parts = []
    for q in range(halfp // LANES):
        cols = slice(q * LANES, (q + 1) * LANES)
        at_u = jnp.broadcast_to(jnp.maximum(u_m[:, cols], 0), (boards, LANES))
        at_v = jnp.broadcast_to(jnp.maximum(v_m[:, cols], 0), (boards, LANES))
        taken_parts.append(lookup(totals, at_u) + lookup(totals, at_v))
    taken = jnp.concatenate(taken_parts, axis=1)
    live = 0.5 * jnp.sum(totals, axis=1, keepdims=True) - taken[:, :half] + opp[...].astype(F32)
    half_pot = 0.5 * column(pot[...])
    win = half_pot + column(bet[...] * pot[...])
    stake = half_pot * live * (1.0 / hands)

    m_copy.wait()
    value = jnp.maximum(win * mm[:, :half] * (1.0 / hands), -stake)
    bv_out[...] = value
    scale = 1.0 / (boards * nb)
    hand_part = jnp.sum(value, axis=0, keepdims=True) * scale
    mass_part = jnp.sum(stake, axis=0, keepdims=True) * scale
    tr = trav[...].reshape(1, half)
    num = jnp.sum(tr * hand_part, axis=1, keepdims=True)
    den = jnp.sum(tr * mass_part, axis=1, keepdims=True)
    lane = iota((1, halfp), 1)
    msg[...] = jnp.where(lane == halfp - 2, num, jnp.where(lane == halfp - 1, den, 0.0))
    msg[:, :half] = hand_part

    copies = []
    for k in range(nb):
        peer = lax.rem(me + k, nb)
        if k:
            copies.append(
                pltpu.make_async_remote_copy(
                    src_ref=msg, dst_ref=recva.at[k], send_sem=send_a.at[k], recv_sem=recv_a.at[k],
                    device_id=(peer, h), device_id_type=MESH,
                )
            )
        copies.append(
            pltpu.make_async_remote_copy(
                src_ref=msg.at[:, pl.ds(halfp - LANES, LANES)], dst_ref=recvb.at[k],
                send_sem=send_b.at[k], recv_sem=recv_b.at[k],
                device_id=(peer, 1 - h), device_id_type=MESH,
            )
        )
    for copy in copies:
        copy.start()
    for copy in copies:
        copy.wait()
    total = msg[...]
    tail = jnp.zeros((1, LANES), F32)
    for k in range(nb):
        if k:
            total = total + recva[k]
        tail = tail + recvb[k]
    hv_out[...] = total[:, :half].reshape(half)
    ends = total[:, halfp - LANES :] + tail
    spot = iota((1, LANES), 1)
    num_all = jnp.sum(jnp.where(spot == LANES - 2, ends, 0.0), axis=1, keepdims=True)
    den_all = jnp.sum(jnp.where(spot == LANES - 1, ends, 0.0), axis=1, keepdims=True)
    ex_out[...] = num_all / den_all


def solution(mesh):
    nb = mesh.shape["board"]

    def local(opp_reach, hand_rank, hand_cards, pot, bet_frac, trav_reach):
        boards, half = opp_reach.shape
        hands = hand_rank.shape[1]
        own = boards // 2
        hp = up(hands, LANES)
        halfp = up(half + 2, LANES)
        blocks = -(-(CARDS // 2) // (LANES // own))
        nhi = up(-(-hands // DIGIT), 16)
        nlo = DIGIT + 16
        vm = pltpu.VMEM
        dma = pltpu.SemaphoreType.DMA
        spec = pl.BlockSpec(memory_space=pltpu.VMEM)
        value, hand_values, ratio = pl.pallas_call(
            functools.partial(kernel, nb),
            out_shape=(vm((boards, half), F32), vm((half,), F32), vm((1, 1), F32)),
            in_specs=[spec] * 6,
            scratch_shapes=[
                vm((CARDS * STRIDE, hp), BF16),
                vm((2, hp), jnp.int32),
                vm((own, hp), F32),
                vm((own, hp), F32),
                vm((own, hp), F32),
                vm((3 * own, hp), BF16),
                vm((own, half), BF16),
                vm((blocks, LANES, LANES), F32),
                vm((blocks, LANES, LANES), F32),
                vm((blocks, LANES, LANES), F32),
                vm((own, 2 * nhi, hp), BF16),
                vm((own, nlo, 2 * nhi), F32),
                vm((own, 2 * nhi), F32),
                vm((own, hp), F32),
                vm((boards, LANES), F32),
                vm((boards, halfp), F32),
                vm((own, halfp), F32),
                vm((1, halfp), F32),
                vm((nb, 1, halfp), F32),
                vm((nb, 1, LANES), F32),
                dma((2,)),
                dma((2,)),
                dma((2,)),
                dma((nb,)),
                dma((nb,)),
                dma((nb,)),
                dma((nb,)),
            ],
            compiler_params=pltpu.CompilerParams(collective_id=0, has_side_effects=True),
        )(opp_reach, hand_rank, hand_cards.T, pot[None, :], bet_frac[None, :], trav_reach)
        return value, hand_values, ratio[0, 0]

    placed = (P("board", "hand"), P("board", None), P(), P("board"), P("board"), P("hand"))
    return jax.shard_map(
        local,
        mesh=mesh,
        in_specs=placed,
        out_specs=(P("board", "hand"), P("hand"), P()),
        check_vma=False,
    )
```

```python
import functools

import jax
import jax.numpy as jnp
from jax import lax
from jax.experimental import pallas as pl
from jax.experimental.pallas import tpu as pltpu
from jax.sharding import PartitionSpec as P

CARDS = 52
LANES = 128
SLOT = 64
EACH = CARDS - 1
FOLD = CARDS // 2
PAIRS = FOLD // 2
ROWS = 56
BATCH = 8
MIDDLE = 662.0
DIGIT = 32
TOPS = 42
UNIT = 8192.0
WBITS = 14
RBITS = 11
MESH = pl.DeviceIdType.MESH
F32 = jnp.float32
BF16 = jnp.bfloat16
I32 = jnp.int32
NT = (((1,), (1,)), ((), ()))


def up(n, m):
    return (n + m - 1) // m * m


def iota(shape, axis, dtype=I32):
    return lax.broadcasted_iota(I32, shape, axis).astype(dtype)


def lookup(table, at):
    return jnp.take_along_axis(table, at, axis=1, mode="promise_in_bounds")


def spread(row, rows=8):
    return jnp.broadcast_to(row, (rows, row.shape[1]))


def column(row):
    n = row.shape[1]
    diag = iota((n, n), 0) == iota((n, n), 1)
    return jnp.sum(jnp.where(diag, row, 0.0), axis=1, keepdims=True)


def split3(x):
    top = x.astype(BF16)
    rest = x - top.astype(F32)
    mid = rest.astype(BF16)
    return top, mid, (rest - mid.astype(F32)).astype(BF16)


def join(ref, left, first, second):
    half = first.shape[1]
    ref[...] = jnp.zeros(ref.shape, F32)
    ref[:, :half] = jnp.where(left, second, first)
    back = pltpu.roll(ref[...], half, 1)
    ref[...] = jnp.zeros(ref.shape, F32)
    ref[:, :half] = jnp.where(left, first, second)
    ref[...] = ref[...] + back


def folded(u, v):
    low = u < FOLD
    row_x, slot_x = jnp.where(low, u, EACH - u), jnp.where(low, v - u - 1, v - 1)
    low = v < FOLD
    row_y, slot_y = jnp.where(low, v, EACH - v), jnp.where(low, u + EACH - v, u)
    return (row_x >> 1, SLOT * (row_x & 1) + slot_x), (row_y >> 1, SLOT * (row_y & 1) + slot_y)


def gathered(src, pat, k, groups, width):
    top, low = spread(pat[k : k + 1, :]), spread(pat[32 + k : 33 + k, :])
    accs = [jnp.zeros((8, LANES), I32) for _ in range(groups)]
    for s in range(width // LANES):
        here = top == s
        for g in range(groups):
            piece = src[8 * g : 8 * g + 8, s * LANES : (s + 1) * LANES]
            accs[g] = jnp.where(here, lookup(piece, low), accs[g])
    return accs


def first_part(j, rows):
    quad = iota((rows, LANES), 0) >> 5
    lane = iota((rows, LANES), 1)
    row = 8 * j + 2 * quad + (lane >> 6)
    return (lane & (SLOT - 1)) < EACH - row


def kernel(
    nb, opp, rank, cards, pot, bet, trav, bv_out, hv_out, ex_out,
    cards_s, rank_s, opp_s, opp_t, got, tra, trb, pots, bets, uv, rk, wf, trf, scal, pat, r2, xy,
    tt, up_t, dn_t, st, sx, c1, ft, hib, lob, pk, vals, parts, sbuf, msg, recv,
    sem, s_x, s_t, s_v, send, arrive,
):
    me, h = lax.axis_index("board"), lax.axis_index("hand")
    boards, half = opp.shape
    hands = rank.shape[1]
    own = boards // 2
    hp = wf.shape[1]
    wide = msg.shape[2]
    groups = own // 8
    mine = pl.multiple_of(h * own, own)
    theirs = pl.multiple_of((1 - h) * own, own)
    partner = (me, 1 - h)
    left = h == 0
    barrier = pltpu.get_barrier_semaphore()
    for k in range(nb):
        peer = lax.rem(me + k, nb)
        if k:
            pl.semaphore_signal(barrier, inc=1, device_id=(peer, h), device_id_type=MESH)
        pl.semaphore_signal(barrier, inc=1, device_id=(peer, 1 - h), device_id_type=MESH)
    loads = [
        pltpu.make_async_copy(cards, cards_s, sem.at[0]),
        pltpu.make_async_copy(rank.at[pl.ds(mine, own)], rank_s, sem.at[1]),
        pltpu.make_async_copy(opp.at[pl.ds(theirs, own)], opp_t, sem.at[2]),
        pltpu.make_async_copy(trav, tra, sem.at[3]),
        pltpu.make_async_copy(pot, pots, sem.at[4]),
        pltpu.make_async_copy(bet, bets, sem.at[5]),
        pltpu.make_async_copy(opp.at[pl.ds(mine, own)], opp_s, sem.at[6]),
    ]
    for copy in loads:
        copy.start()

    loads[0].wait()
    uv[...] = jnp.full(uv.shape, -1, I32)
    uv[:, :hands] = cards_s[...]
    u, v = uv[0:1, :], uv[1:2, :]
    lane = iota((1, hp), 1)
    at_top, at_low = (lane // LANES + 1).astype(F32), (lane % LANES).astype(F32)
    pair = iota((16, hp), 0)
    spot = iota((LANES, hp), 0, F32).astype(BF16)
    for q, (prow, plane) in enumerate(folded(u, v)):
        in_pair = pair == prow
        lhs = jnp.concatenate([jnp.where(in_pair, at_top, 0.0), jnp.where(in_pair, at_low, 0.0)], axis=0)
        rhs = jnp.where(spot == spread(plane.astype(F32).astype(BF16), LANES), jnp.ones((), BF16), jnp.zeros((), BF16))
        index = lax.dot_general(lhs.astype(BF16), rhs, NT, preferred_element_type=F32).astype(I32)
        pat[16 * q : 16 * q + 16, :] = index[0:16] - 1
        pat[32 + 16 * q : 48 + 16 * q, :] = index[16:32]

    loads[1].wait()
    rk[...] = jnp.zeros(rk.shape, I32)
    rk[:, :hands] = rank_s[...]
    r2[...] = rk[0:16, :] + (rk[16:32, :] << RBITS)
    for q in range(2):
        for p in range(PAIRS):
            for g, both in enumerate(gathered(r2, pat, 16 * q + p, 2, hp)):
                row = p * 32 + 8 * g
                xy[q, row : row + 8, :] = (both & ((1 << RBITS) - 1)) << WBITS
                xy[q, row + 16 : row + 24, :] = (both >> RBITS) << WBITS
    hib[...] = (rk[...] >> 5).astype(F32)
    lob[...] = (rk[...] & (DIGIT - 1)).astype(F32)
    loads[4].wait()
    loads[5].wait()
    half_pot = 0.5 * column(pots[...])
    win = half_pot + column(bets[...] * pots[...])
    scal[0:own, :] = jnp.broadcast_to(jnp.where(left, win[0:own], win[own:]) * (1.0 / hands), (own, LANES))
    scal[own:, :] = jnp.broadcast_to(jnp.where(left, half_pot[0:own], half_pot[own:]) * (1.0 / hands), (own, LANES))
    loads[2].wait()
    loads[3].wait()

    pl.semaphore_wait(barrier, 2 * nb - 1)
    x_copy = pltpu.make_async_remote_copy(
        src_ref=opp_t, dst_ref=got, send_sem=s_x.at[0], recv_sem=s_x.at[1],
        device_id=partner, device_id_type=MESH,
    )
    x_copy.start()
    t_copy = pltpu.make_async_remote_copy(
        src_ref=tra, dst_ref=trb, send_sem=s_t.at[0], recv_sem=s_t.at[1],
        device_id=partner, device_id_type=MESH,
    )
    t_copy.start()
    loads[6].wait()
    t_copy.wait()
    join(trf, left, tra[...].reshape(1, half), trb[...].reshape(1, half))
    x_copy.wait()
    join(wf, left, opp_s[...].astype(F32), got[...].astype(F32))

    wi = (wf[...] * UNIT).astype(I32)
    r2[...] = wi[0:16] + (wi[16:32] << WBITS)
    for q in range(2):
        for p in range(PAIRS):
            for g, both in enumerate(gathered(r2, pat, 16 * q + p, 2, hp)):
                row = p * 32 + 8 * g
                xy[q, row : row + 8, :] = xy[q, row : row + 8, :] + (both & ((1 << WBITS) - 1))
                xy[q, row + 16 : row + 24, :] = xy[q, row + 16 : row + 24, :] + (both >> WBITS)

    def load_block(n, packed):
        rows = slice(n * LANES, n * LANES + packed.shape[1])
        both = packed.T
        t = (both >> WBITS).astype(F32) - MIDDLE
        w = (both & ((1 << WBITS) - 1)).astype(F32) * (1.0 / UNIT)
        tt[rows, :] = t[: packed.shape[1]]
        up_t[rows, :] = (t + w)[: packed.shape[1]]
        dn_t[rows, :] = (t - w)[: packed.shape[1]]

    full = PAIRS // 4
    for j in range(full):
        rows = slice(j * LANES, (j + 1) * LANES)
        part = first_part(j, LANES)
        x, y = xy[0, rows, :], xy[1, rows, :]
        load_block(2 * j, jnp.where(part, x, y))
        load_block(2 * j + 1, jnp.where(part, y, x))
    rest = slice(full * LANES, full * LANES + 32)
    part = first_part(full, 32)
    x, y = xy[0, rest, :], xy[1, rest, :]
    lo_r, hi_r = jnp.where(part, x, y), jnp.where(part, y, x)
    load_block(2 * full, jnp.concatenate([lo_r, pltpu.roll(lo_r, SLOT, 1), hi_r, pltpu.roll(hi_r, SLOT, 1)], axis=0))

    halves = 4 * full + 1

    def pairwise(n):
        base = n * SLOT if isinstance(n, int) else pl.multiple_of(n * SLOT, SLOT)
        here = tt[pl.ds(base, ROWS), :]
        acc = jnp.zeros((ROWS, LANES), F32)
        for e0 in range(0, EACH, BATCH):
            size = min(BATCH, EACH - e0)
            pieces = []
            for e in range(e0, e0 + size):
                pieces.append(jnp.minimum(jnp.maximum(here, dn_t[pl.ds(base + e, 1), :]), up_t[pl.ds(base + e, 1), :]))
            while len(pieces) > 1:
                pieces = [a + b for a, b in zip(pieces[::2], pieces[1::2])] + pieces[len(pieces) // 2 * 2 :]
            base_sum = tt[pl.ds(base + e0, 1), :]
            for e in range(e0 + 1, e0 + size):
                base_sum = base_sum + tt[pl.ds(base + e, 1), :]
            acc = acc + (pieces[0] - base_sum)
        st[pl.ds(base, ROWS), :] = acc

    nhi = up(TOPS, 16)
    hi_row = iota((nhi, hp), 0, F32).astype(BF16)
    lo_row = iota((DIGIT, hp), 0, F32).astype(BF16)

    def hist(b):
        hi_b = spread(hib[pl.ds(b, 1), :].astype(BF16), nhi)
        lo_b = spread(lob[pl.ds(b, 1), :].astype(BF16), DIGIT)
        w_b = spread(wf[pl.ds(b, 1), :].astype(BF16), DIGIT)
        eq = jnp.where(hi_row == hi_b, jnp.ones((), BF16), jnp.zeros((), BF16))
        lw = jnp.where(lo_b <= lo_row, w_b, jnp.zeros((), BF16))
        start = b * DIGIT if isinstance(b, int) else pl.multiple_of(b * DIGIT, DIGIT)
        c1[pl.ds(start, DIGIT), 0:nhi] = lax.dot_general(lw, eq, NT, preferred_element_type=F32)

    st[...] = jnp.zeros(st.shape, F32)

    def both_loop(i, carry):
        for k in range(full):
            pairwise(full * i + k)
        for k in range(8):
            hist(8 * i + k)
        return carry

    lax.fori_loop(0, groups, both_loop, 0)
    pairwise(halves - 1)

    for j in range(full):
        rows = slice(j * LANES, (j + 1) * LANES)
        part = first_part(j, LANES)
        lo_r, hi_r = st[2 * j * LANES : (2 * j + 1) * LANES, :].T, st[(2 * j + 1) * LANES : (2 * j + 2) * LANES, :].T
        sx[0, rows, :] = jnp.where(part, lo_r, hi_r)
        sx[1, rows, :] = jnp.where(part, hi_r, lo_r)
    last = st[2 * full * LANES : (2 * full + 1) * LANES, :].T
    at_left = iota((32, LANES), 1) < SLOT
    lo_r = jnp.where(at_left, last[0:32], pltpu.roll(last[32:64], SLOT, 1))
    hi_r = jnp.where(at_left, last[64:96], pltpu.roll(last[96:128], SLOT, 1))
    part = first_part(full, 32)
    sx[0, rest, :] = jnp.where(part, lo_r, hi_r)
    sx[1, rest, :] = jnp.where(part, hi_r, lo_r)

    lanes = iota((8, LANES), 1)
    sums = jnp.where(iota((own, LANES), 1) < TOPS, c1[pl.ds(DIGIT - 1, own, stride=DIGIT), :], 0.0)
    a, z = iota((LANES, LANES), 0), iota((LANES, LANES), 1)
    sgn = jnp.where(z > a, 1, jnp.where(z < a, -1, 0)).astype(F32).astype(BF16)
    coarse = -sums
    for piece in split3(sums):
        coarse = coarse + jnp.dot(piece, sgn, preferred_element_type=F32)
    for g in range(groups):
        base = coarse[8 * g : 8 * g + 8]
        below = jnp.zeros((8, LANES), F32)
        row = []
        for lo in range(DIGIT):
            upto = c1[pl.ds(g * 8 * DIGIT + lo, 8, stride=DIGIT), :]
            row.append(base + below + upto)
            below = upto
        for s in range(up(DIGIT, 3) // 3):
            out = row[3 * s]
            for q in range(1, 3):
                if 3 * s + q < DIGIT:
                    out = jnp.where(lanes < q * TOPS, out, pltpu.roll(row[3 * s + q], q * TOPS, 1))
            ft[8 * g : 8 * g + 8, s * LANES : (s + 1) * LANES] = out

    card_row = iota((LANES, hp), 0)
    u, v = uv[0:1, :], uv[1:2, :]
    hold = ((card_row == u) | (card_row == v)).astype(F32).astype(BF16)
    taken = lax.dot_general(wf[...].astype(BF16), hold, NT, preferred_element_type=F32)
    whole = 0.5 * jnp.sum(taken, axis=1, keepdims=True)

    for c in range(hp // LANES):
        cols = slice(c * LANES, (c + 1) * LANES)
        uc, vc = uv[0:1, cols], uv[1:2, cols]
        corr = [jnp.zeros((8, LANES), F32) for _ in range(groups)]
        for q, (prow, plane) in enumerate(folded(uc, vc)):
            top, low = spread(prow), spread(plane)
            accs = [jnp.zeros((8, LANES), F32) for _ in range(groups)]
            for p in range(PAIRS):
                here = top == p
                for g in range(groups):
                    accs[g] = jnp.where(here, lookup(sx[q, p * 32 + 8 * g : p * 32 + 8 * g + 8, :], low), accs[g])
            corr = [x + y for x, y in zip(corr, accs)]
        ua, va = spread(jnp.maximum(uc, 0)), spread(jnp.maximum(vc, 0))
        part = jnp.zeros((8, LANES), F32)
        mass = jnp.zeros((8, LANES), F32)
        for g in range(groups):
            rows = slice(8 * g, 8 * g + 8)
            r = rk[rows, cols]
            lo = r & (DIGIT - 1)
            top = (lo * 43) >> 7
            low = (lo - 3 * top) * TOPS + (r >> 5)
            pick = jnp.zeros((8, LANES), F32)
            for s in range(up(DIGIT, 3) // 3):
                pick = jnp.where(top == s, lookup(ft[rows, s * LANES : (s + 1) * LANES], low), pick)
            margin = pick - corr[g]
            t = taken[rows]
            live = whole[rows] - lookup(t, ua) - lookup(t, va) + wf[rows, cols]
            stake = scal[own + 8 * g : own + 8 * g + 8, :] * live
            value = jnp.maximum(scal[rows, :] * margin, -stake)
            vals[rows, cols] = value
            part = part + value
            mass = mass + stake
        parts[0:1, cols] = jnp.sum(part, axis=0, keepdims=True)
        parts[1:2, cols] = jnp.sum(mass, axis=0, keepdims=True)

    scale = 1.0 / (boards * nb)
    shift = hp - half
    trow = trf[...]
    num = jnp.sum(trow * parts[0:1, :], axis=1, keepdims=True)
    den = jnp.sum(trow * parts[1:2, :], axis=1, keepdims=True)
    spot = iota((1, wide), 1)
    tail = jnp.where(spot == wide - 2, num, jnp.where(spot == wide - 1, den, 0.0))
    both = parts[...]
    msg[0] = jnp.where(spot < half, both[0:1, :wide], tail)
    msg[1] = jnp.where(spot < half, pltpu.roll(both, shift, 1)[0:1, :wide], tail)

    copies = []
    for k in range(nb):
        peer = lax.rem(me + k, nb)
        for q in range(2):
            if k == 0 and q == 0:
                continue
            to = h if q == 0 else 1 - h
            copies.append(
                pltpu.make_async_remote_copy(
                    src_ref=msg.at[to], dst_ref=recv.at[2 * k + q],
                    send_sem=send.at[2 * k + q], recv_sem=arrive.at[2 * k + q],
                    device_id=(peer, to), device_id_type=MESH,
                )
            )
    for copy in copies:
        copy.start()

    first = vals[:, :half]
    second = pltpu.roll(vals[...], shift, 1)[:, :half]
    sbuf[...] = jnp.where(left, second, first)
    v_copy = pltpu.make_async_remote_copy(
        src_ref=sbuf, dst_ref=bv_out.at[pl.ds(mine, own)], send_sem=s_v.at[0], recv_sem=s_v.at[1],
        device_id=(me, 1 - h), device_id_type=MESH,
    )
    v_copy.start()
    bv_out[pl.ds(mine, own), :] = jnp.where(left, first, second)
    for copy in copies:
        copy.wait()
    total = msg[h]
    for k in range(1, 2 * nb):
        total = total + recv[k]
    hv_out[...] = (total[:, :half] * scale).reshape(half)
    num_all = jnp.sum(jnp.where(spot == wide - 2, total, 0.0), axis=1, keepdims=True)
    den_all = jnp.sum(jnp.where(spot == wide - 1, total, 0.0), axis=1, keepdims=True)
    ex_out[...] = num_all / den_all
    v_copy.wait()


def solution(mesh):
    nb = mesh.shape["board"]

    def local(opp_reach, hand_rank, hand_cards, pot, bet_frac, trav_reach):
        boards, half = opp_reach.shape
        hands = hand_rank.shape[1]
        own = boards // 2
        hp = up(hands, LANES)
        wide = up(half + 2, LANES)
        rows = up(PAIRS, 4) * 32
        tall = (2 * (PAIRS // 4) + 1) * LANES
        vm = pltpu.VMEM
        dma = pltpu.SemaphoreType.DMA
        value, hand_values, ratio = pl.pallas_call(
            functools.partial(kernel, nb),
            out_shape=(vm((boards, half), F32), vm((half,), F32), vm((1, 1), F32)),
            in_specs=[pl.BlockSpec(memory_space=pl.ANY)] * 6,
            scratch_shapes=[
                vm((2, hands), I32),
                vm((own, hands), I32),
                vm((own, half), BF16),
                vm((own, half), BF16),
                vm((own, half), BF16),
                vm((half,), F32),
                vm((half,), F32),
                vm((1, boards), F32),
                vm((1, boards), F32),
                vm((2, hp), I32),
                vm((own, hp), I32),
                vm((own, hp), F32),
                vm((1, hp), F32),
                vm((2 * own, LANES), F32),
                vm((64, LANES), I32),
                vm((16, hp), I32),
                vm((2, rows, LANES), I32),
                vm((tall, LANES), F32),
                vm((tall, LANES), F32),
                vm((tall, LANES), F32),
                vm((tall, LANES), F32),
                vm((2, rows, LANES), F32),
                vm((own * DIGIT, LANES), F32),
                vm((own, hp), F32),
                vm((own, hp), F32),
                vm((own, hp), F32),
                vm((own, hp), F32),
                vm((own, hp), F32),
                vm((2, hp), F32),
                vm((own, half), F32),
                vm((2, 1, wide), F32),
                vm((2 * nb, 1, wide), F32),
                dma((7,)),
                dma((2,)),
                dma((2,)),
                dma((2,)),
                dma((2 * nb,)),
                dma((2 * nb,)),
            ],
            compiler_params=pltpu.CompilerParams(collective_id=0, has_side_effects=True),
            name="main",
        )(opp_reach, hand_rank, hand_cards.T, pot[None, :], bet_frac[None, :], trav_reach)
        return value, hand_values, ratio[0, 0]

    placed = (P("board", "hand"), P("board", None), P(), P("board"), P("board"), P("hand"))
    return jax.shard_map(
        local,
        mesh=mesh,
        in_specs=placed,
        out_specs=(P("board", "hand"), P("hand"), P()),
        check_vma=False,
    )
```

```python
import functools

import jax
import jax.numpy as jnp
from jax import lax
from jax.experimental import pallas as pl
from jax.experimental.pallas import tpu as pltpu
from jax.sharding import PartitionSpec as P

CARDS = 52
LANES = 128
SLOT = 64
EACH = CARDS - 1
FOLD = CARDS // 2
PAIRS = FOLD // 2
ROWS = 56
BATCH = 8
MIDDLE = 662.0
LAG = 5
PARTS = ((0, 4), (4, 7))
FIRST = 10
FAR = 1e30
DIGIT = 32
TOPS = 42
UNIT = 8192.0
WBITS = 14
RBITS = 11
MESH = pl.DeviceIdType.MESH
F32 = jnp.float32
BF16 = jnp.bfloat16
I32 = jnp.int32
NT = (((1,), (1,)), ((), ()))


def up(n, m):
    return (n + m - 1) // m * m


def iota(shape, axis, dtype=I32):
    return lax.broadcasted_iota(I32, shape, axis).astype(dtype)


def lookup(table, at):
    return jnp.take_along_axis(table, at, axis=1, mode="promise_in_bounds")


def place(ref, half_ref, left):
    half = half_ref.shape[1]
    ref[...] = jnp.zeros(ref.shape, ref.dtype)
    ref[:, :half] = half_ref[...]
    flat = ref[...].astype(F32)
    ref[...] = jnp.where(left, flat, pltpu.roll(flat, half, 1)).astype(ref.dtype)


def spread(row, rows=8):
    return jnp.broadcast_to(row, (rows, row.shape[1]))


def column(row):
    n = row.shape[1]
    diag = iota((n, n), 0) == iota((n, n), 1)
    return jnp.sum(jnp.where(diag, row, 0.0), axis=1, keepdims=True)


def split3(x):
    top = x.astype(BF16)
    rest = x - top.astype(F32)
    mid = rest.astype(BF16)
    return top, mid, (rest - mid.astype(F32)).astype(BF16)


def join(ref, left, first, second):
    half = first.shape[1]
    ref[...] = jnp.zeros(ref.shape, F32)
    ref[:, :half] = jnp.where(left, second, first)
    back = pltpu.roll(ref[...], half, 1)
    ref[...] = jnp.zeros(ref.shape, F32)
    ref[:, :half] = jnp.where(left, first, second)
    ref[...] = ref[...] + back


def folded(u, v):
    low = u < FOLD
    row_x, slot_x = jnp.where(low, u, EACH - u), jnp.where(low, v - u - 1, v - 1)
    low = v < FOLD
    row_y, slot_y = jnp.where(low, v, EACH - v), jnp.where(low, u + EACH - v, u)
    return (row_x >> 1, SLOT * (row_x & 1) + slot_x), (row_y >> 1, SLOT * (row_y & 1) + slot_y)


def gathered(src, pat, k, groups, width, after=lambda at: at):
    top, low = spread(pat[k : k + 1, :]), after(spread(pat[32 + k : 33 + k, :]))
    accs = [jnp.zeros((8, LANES), I32) for _ in range(groups)]
    for s in range(width // LANES):
        here = top == s
        for g in range(groups):
            piece = src[8 * g : 8 * g + 8, s * LANES : (s + 1) * LANES]
            accs[g] = jnp.where(here, lookup(piece, low), accs[g])
    return accs


def first_part(j, rows):
    quad = iota((rows, LANES), 0) >> 5
    lane = iota((rows, LANES), 1)
    row = 8 * j + 2 * quad + (lane >> 6)
    return (lane & (SLOT - 1)) < EACH - row


def kernel(
    nb, opp, rank, cards, pot, bet, trav, bv_out, hv_out, ex_out,
    cards_s, rank_s, opp_s, opp_t, home, away, got, tra, trb, pots, bets, uv, rk, wf, trf, scal, pat, fold, r2, xy,
    tt, up_t, dn_t, ts, st, sb, sx, c1, ft, hib, lob, ptop, plow, ct, whole, stake, corr, pk, vals, parts, sbuf, msg, recv,
    sem, s_x, s_t, s_v, send, arrive,
):
    me, h = lax.axis_index("board"), lax.axis_index("hand")
    boards, half = opp.shape
    hands = rank.shape[1]
    own = boards // 2
    hp = wf.shape[1]
    wide = msg.shape[2]
    groups = own // 8
    mine = pl.multiple_of(h * own, own)
    theirs = pl.multiple_of((1 - h) * own, own)
    partner = (me, 1 - h)
    left = h == 0
    loads = [
        pltpu.make_async_copy(cards, cards_s, sem.at[0]),
        pltpu.make_async_copy(rank.at[pl.ds(mine, own)], rank_s, sem.at[1]),
        pltpu.make_async_copy(opp.at[pl.ds(theirs, own)], opp_t, sem.at[2]),
        pltpu.make_async_copy(trav, tra, sem.at[3]),
        pltpu.make_async_copy(pot, pots, sem.at[4]),
        pltpu.make_async_copy(bet, bets, sem.at[5]),
        pltpu.make_async_copy(opp.at[pl.ds(mine, own)], opp_s, sem.at[6]),
    ]
    for copy in loads:
        copy.start()
    barrier = pltpu.get_barrier_semaphore()
    for k in range(nb):
        peer = lax.rem(me + k, nb)
        if k:
            pl.semaphore_signal(barrier, inc=1, device_id=(peer, h), device_id_type=MESH)
        pl.semaphore_signal(barrier, inc=1, device_id=(peer, 1 - h), device_id_type=MESH)
    loads[0].wait()
    uv[...] = jnp.full(uv.shape, -1, I32)
    uv[:, :hands] = cards_s[...]
    u, v = uv[0:1, :], uv[1:2, :]
    lane = iota((1, hp), 1)
    at_top, at_low = (lane // LANES + 1).astype(F32), (lane % LANES).astype(F32)
    pair = iota((16, hp), 0)
    spot = iota((LANES, hp), 0, F32).astype(BF16)
    for q, (prow, plane) in enumerate(folded(u, v)):
        fold[2 * q : 2 * q + 1, :] = prow
        fold[2 * q + 1 : 2 * q + 2, :] = plane
        in_pair = pair == prow
        lhs = jnp.concatenate([jnp.where(in_pair, at_top, 0.0), jnp.where(in_pair, at_low, 0.0)], axis=0)
        rhs = jnp.where(spot == spread(plane.astype(F32).astype(BF16), LANES), jnp.ones((), BF16), jnp.zeros((), BF16))
        index = lax.dot_general(lhs.astype(BF16), rhs, NT, preferred_element_type=F32).astype(I32)
        pat[16 * q : 16 * q + 16, :] = index[0:16] - 1
        pat[32 + 16 * q : 48 + 16 * q, :] = index[16:32]
    fold[4:6, :] = jnp.maximum(uv[...], 0)
    loads[2].wait()
    loads[3].wait()
    place(away, opp_t, left)
    loads[6].wait()
    place(home, opp_s, left)
    loads[4].wait()
    loads[5].wait()
    half_pot = 0.5 * column(pots[...])
    win = half_pot + column(bets[...] * pots[...])
    scal[0:own, :] = jnp.broadcast_to(jnp.where(left, win[0:own], win[own:]) * (1.0 / hands), (own, LANES))
    scal[own:, :] = jnp.broadcast_to(jnp.where(left, half_pot[0:own], half_pot[own:]) * (1.0 / hands), (own, LANES))

    pl.semaphore_wait(barrier, 2 * nb - 1)
    x_copy = pltpu.make_async_remote_copy(
        src_ref=away, dst_ref=got, send_sem=s_x.at[0], recv_sem=s_x.at[1],
        device_id=partner, device_id_type=MESH,
    )
    x_copy.start()
    t_copy = pltpu.make_async_remote_copy(
        src_ref=tra, dst_ref=trb, send_sem=s_t.at[0], recv_sem=s_t.at[1],
        device_id=partner, device_id_type=MESH,
    )
    t_copy.start()

    loads[1].wait()
    rk[...] = jnp.zeros(rk.shape, I32)
    rk[:, :hands] = rank_s[...]
    r2[...] = rk[0:16, :] + (rk[16:32, :] << RBITS)
    columns = hp // LANES
    full = PAIRS // 4
    rest = slice(full * LANES, full * LANES + 32)
    nhi = up(TOPS, 16)
    steps = up(DIGIT, 3) // 3
    hi_row = iota((nhi, hp), 0, F32).astype(BF16)
    lo_row = iota((DIGIT, hp), 0, F32).astype(BF16)

    def digits(c):
        cols = slice(c * LANES, (c + 1) * LANES)
        r = rk[:, cols]
        lo, hi = r & (DIGIT - 1), r >> 5
        top = (lo * 43) >> 7
        hib[:, cols] = hi.astype(F32)
        lob[:, cols] = lo.astype(F32)
        ptop[:, cols] = top
        plow[:, cols] = (lo - 3 * top) * TOPS + hi

    def stretch(ref, b, rows):
        tile = spread(ref[b : b + 1, :], 16).astype(BF16)
        return jnp.concatenate([tile] * (rows // 16), axis=0)

    def gather_rank(p, q):
        for g, both in enumerate(gathered(r2, pat, 16 * q + p, 2, hp)):
            row = p * 32 + 8 * g
            xy[q, row : row + 8, :] = (both & ((1 << RBITS) - 1)) << WBITS
            xy[q, row + 16 : row + 24, :] = (both >> RBITS) << WBITS

    def weave(streams):
        most = max(len(x) for x in streams)
        done = [0] * len(streams)
        for i in range(1, most + 1):
            for k, stream in enumerate(streams):
                while done[k] * most < i * len(stream):
                    stream[done[k]]()
                    done[k] += 1

    def run(*streams):
        run_each([streams])

    def run_each(groups_of):
        def body(i, carry):
            passed.clear()
            for streams in groups_of:
                weave(streams)
            passed.clear()
            return carry

        lax.fori_loop(0, once, body, 0)

    passed = []
    once = 1 + me // nb
    make = functools.partial
    weave([[make(digits, c) for c in range(columns)]])
    run([make(gather_rank, p, q) for p in range(PAIRS) for q in range(2)])
    t_copy.wait()
    x_copy.wait()
    wf[...] = home[...].astype(F32) + got[...].astype(F32)
    wi = (wf[...] * UNIT).astype(I32)
    r2[...] = wi[0:16] + (wi[16:32] << WBITS)

    def after(at):
        if len(passed) < LAG:
            return at
        return jnp.where(passed[-LAG] > FAR, 0, at)

    def gather(p, q):
        for g, both in enumerate(gathered(r2, pat, 16 * q + p, 2, hp, after)):
            row = p * 32 + 8 * g
            xy[q, row : row + 8, :] = xy[q, row : row + 8, :] + (both & ((1 << WBITS) - 1))
            xy[q, row + 16 : row + 24, :] = xy[q, row + 16 : row + 24, :] + (both >> WBITS)

    def load_rows(n, packed):
        rows = slice(n * LANES, (n + 1) * LANES)
        both = packed.T
        t = (both >> WBITS).astype(F32) - MIDDLE
        w = (both & ((1 << WBITS) - 1)).astype(F32) * (1.0 / UNIT)
        tt[rows, :] = t
        up_t[rows, :] = t + w
        dn_t[rows, :] = t - w
        slot = iota((LANES, LANES), 0) & (SLOT - 1)
        sums = jnp.sum(jnp.where(slot < EACH, t, 0.0).reshape(LANES // BATCH, BATCH, LANES), axis=1)
        ts[n * (LANES // BATCH) : (n + 1) * (LANES // BATCH), :] = sums

    def load_block(j, side):
        if j < full:
            rows = slice(j * LANES, (j + 1) * LANES)
            part = first_part(j, LANES)
            load_rows(2 * j + side, jnp.where(part, xy[side, rows, :], xy[1 - side, rows, :]))
        else:
            part = first_part(full, 32)
            x, y = xy[0, rest, :], xy[1, rest, :]
            lo_r, hi_r = jnp.where(part, x, y), jnp.where(part, y, x)
            load_rows(2 * full, jnp.concatenate([lo_r, pltpu.roll(lo_r, SLOT, 1), hi_r, pltpu.roll(hi_r, SLOT, 1)], axis=0))

    def pair_tasks(n):
        base = n * SLOT
        state = []

        def step(d0, d1, e0):
            mine_rows = slice(base + 8 * d0, base + 8 * d1)
            here = tt[mine_rows, :]
            size = min(BATCH, EACH - e0)
            at = (base + e0) // BATCH
            some = None
            for e in range(base + e0, base + e0 + size):
                piece = jnp.minimum(jnp.maximum(here, dn_t[e : e + 1, :]), up_t[e : e + 1, :])
                some = piece - ts[at : at + 1, :] if some is None else some + piece
            passed.append(some[0:8])
            acc = state.pop() + some if e0 else some
            if e0 + size == EACH:
                st[mine_rows, :] = acc
                if d0 == 0:
                    st[base + ROWS : base + SLOT, :] = jnp.zeros((SLOT - ROWS, LANES), F32)
            else:
                state.append(acc)

        return [make(step, d0, d1, e0) for d0, d1 in PARTS for e0 in range(0, EACH, BATCH)]

    def hist(b):
        eq = jnp.where(hi_row == stretch(hib, b, nhi), jnp.ones((), BF16), jnp.zeros((), BF16))
        lw = jnp.where(stretch(lob, b, DIGIT) <= lo_row, stretch(wf, b, DIGIT), jnp.zeros((), BF16))
        if b < FIRST:
            passed.append(lw[0:16, 0:LANES].astype(F32)[0:8])
        c1[b * DIGIT : (b + 1) * DIGIT, 0:nhi] = lax.dot_general(lw, eq, NT, preferred_element_type=F32)

    lanes = iota((8, LANES), 1)
    a, z = iota((LANES, LANES), 0), iota((LANES, LANES), 1)
    sgn = jnp.where(z > a, 1, jnp.where(z < a, -1, 0)).astype(F32).astype(BF16)

    def table(g):
        sums = jnp.where(lanes < TOPS, c1[pl.ds(g * 8 * DIGIT + DIGIT - 1, 8, stride=DIGIT), :], 0.0)
        base = -sums
        for piece in split3(sums):
            base = base + jnp.dot(piece, sgn, preferred_element_type=F32)
        below = jnp.zeros((8, LANES), F32)
        row = []
        for lo in range(DIGIT):
            upto = c1[pl.ds(g * 8 * DIGIT + lo, 8, stride=DIGIT), :]
            row.append(base + (below + upto))
            below = upto
        for s in range(steps):
            out = row[3 * s]
            for q in range(1, 3):
                if 3 * s + q < DIGIT:
                    out = jnp.where(lanes < q * TOPS, out, pltpu.roll(row[3 * s + q], q * TOPS, 1))
            ft[8 * g : 8 * g + 8, s * LANES : (s + 1) * LANES] = out

    def pick(g, c):
        rows, cols = slice(8 * g, 8 * g + 8), slice(c * LANES, (c + 1) * LANES)
        top, low = ptop[rows, cols], after(plow[rows, cols])
        out = jnp.zeros((8, LANES), F32)
        for s in range(steps):
            out = jnp.where(top == s, lookup(ft[rows, s * LANES : (s + 1) * LANES], low), out)
        pk[rows, cols] = out

    def totals():
        card_row = iota((LANES, hp), 0)
        hold = ((card_row == uv[0:1, :]) | (card_row == uv[1:2, :])).astype(F32).astype(BF16)
        taken = lax.dot_general(wf[...].astype(BF16), hold, NT, preferred_element_type=F32)
        ct[...] = taken
        whole[...] = jnp.broadcast_to(0.5 * jnp.sum(taken, axis=1, keepdims=True), (own, LANES))

    def stakes(c):
        cols = slice(c * LANES, (c + 1) * LANES)
        ua, va = spread(fold[4:5, cols]), spread(fold[5:6, cols])
        for g in range(groups):
            rows = slice(8 * g, 8 * g + 8)
            t = ct[rows, :]
            live = whole[rows, :] - lookup(t, ua) - lookup(t, va) + wf[rows, cols]
            stake[rows, cols] = scal[own + 8 * g : own + 8 * g + 8, :] * live

    def back(j, side):
        if j < full:
            rows = slice((2 * j + side) * LANES, (2 * j + side + 1) * LANES)
            sb[side] = st[rows, :].T
            if side:
                out = slice(j * LANES, (j + 1) * LANES)
                part = first_part(j, LANES)
                sx[0, out, :] = jnp.where(part, sb[0], sb[1])
                sx[1, out, :] = jnp.where(part, sb[1], sb[0])
        else:
            last = st[2 * full * LANES : (2 * full + 1) * LANES, :].T
            at_left = iota((32, LANES), 1) < SLOT
            lo_r = jnp.where(at_left, last[0:32], pltpu.roll(last[32:64], SLOT, 1))
            hi_r = jnp.where(at_left, last[64:96], pltpu.roll(last[96:128], SLOT, 1))
            part = first_part(full, 32)
            sx[0, rest, :] = jnp.where(part, lo_r, hi_r)
            sx[1, rest, :] = jnp.where(part, hi_r, lo_r)

    def scatter(j, c, stop):
        cols = slice(c * LANES, (c + 1) * LANES)
        out = [None] * groups
        for q in range(2):
            top, low = spread(fold[2 * q : 2 * q + 1, cols]), after(spread(fold[2 * q + 1 : 2 * q + 2, cols]))
            accs = [jnp.zeros((8, LANES), F32) for _ in range(groups)]
            for p in range(4 * j, stop):
                here = top == p
                for g in range(groups):
                    accs[g] = jnp.where(here, lookup(sx[q, p * 32 + 8 * g : p * 32 + 8 * g + 8, :], low), accs[g])
            out = [y if x is None else x + y for x, y in zip(out, accs)]
        return out

    def scatter_add(j, c):
        cols = slice(c * LANES, (c + 1) * LANES)
        for g, x in enumerate(scatter(j, c, 4 * j + 4)):
            rows = slice(8 * g, 8 * g + 8)
            corr[rows, cols] = x if j == 0 else corr[rows, cols] + x

    def finish(c):
        cols = slice(c * LANES, (c + 1) * LANES)
        part = jnp.zeros((8, LANES), F32)
        mass = jnp.zeros((8, LANES), F32)
        for g, x in enumerate(scatter(full - 1, c, PAIRS)):
            rows = slice(8 * g, 8 * g + 8)
            margin = pk[rows, cols] - (corr[rows, cols] + x)
            held = stake[rows, cols]
            value = jnp.maximum(scal[rows, :] * margin, -held)
            vals[rows, cols] = value
            part = part + value
            mass = mass + held
        parts[0:1, cols] = jnp.sum(part, axis=0, keepdims=True)
        parts[1:2, cols] = jnp.sum(mass, axis=0, keepdims=True)

    gathers = lambda j: [make(gather, p, q) for p in range(4 * j, min(4 * j + 4, PAIRS)) for q in range(2)]
    loads_of = lambda j: [make(load_block, j, side) for side in range(2 if j < full else 1)]
    pairs = lambda j: [t for n in range(4 * j, 4 * j + (4 if j < full else 1)) for t in pair_tasks(n)]
    backs = lambda j: [make(back, j, side) for side in range(2 if j < full else 1)]
    hists = lambda g: [make(hist, b) for b in range(8 * g, 8 * g + 8)]
    picks = lambda g: [make(table, g)] + [make(pick, g, c) for c in range(columns)]
    adds = lambda j: [make(scatter_add, j, c) for c in range(columns)]

    bins = [make(hist, b) for b in range(own)]
    reads = [t for g in range(groups) for t in picks(g)]
    run([totals] + gathers(0) + loads_of(0), bins[:FIRST])
    held = [make(stakes, c) for c in range(columns)]
    later = gathers(2) + gathers(3)
    add0, add1 = adds(0), adds(1)
    moves = [
        gathers(1)[:4],
        gathers(1)[4:],
        loads_of(1) + later[:4],
        later[4:8],
        backs(0) + later[8:],
        loads_of(2) + add0[:3],
        loads_of(3) + add0[3:6],
        add0[6:9],
        backs(1) + add0[9:],
        add1[:3],
        add1[3:6],
        add1[6:9],
        backs(2) + add1[9:],
    ]
    more = [10, 13, 16, 19, 22, 24, 26, 28, 30, 32, 32, 32, 32, 32]
    look = [0, 1, 4, 7, 12, 13, 17, 21, 25, 29, 33, 37, 42, 48]
    for span in (range(0, 4), range(4, 8), range(8, 4 * full + 1)):
        run_each([(moves[k] + reads[look[k] : look[k + 1]] + held[k : k + 1], pair_tasks(k), bins[more[k] : more[k + 1]]) for k in span])
    run(backs(3), [make(finish, c) for c in range(columns)])
    join(trf, left, tra[...].reshape(1, half), trb[...].reshape(1, half))

    scale = 1.0 / (boards * nb)
    shift = hp - half
    trow = trf[...]
    num = jnp.sum(trow * parts[0:1, :], axis=1, keepdims=True)
    den = jnp.sum(trow * parts[1:2, :], axis=1, keepdims=True)
    spot = iota((1, wide), 1)
    tail = jnp.where(spot == wide - 2, num, jnp.where(spot == wide - 1, den, 0.0))
    both = parts[...]
    msg[0] = jnp.where(spot < half, both[0:1, :wide], tail)
    msg[1] = jnp.where(spot < half, pltpu.roll(both, shift, 1)[0:1, :wide], tail)

    copies = []
    for k in range(nb):
        peer = lax.rem(me + k, nb)
        for q in range(2):
            if k == 0 and q == 0:
                continue
            to = h if q == 0 else 1 - h
            copies.append(
                pltpu.make_async_remote_copy(
                    src_ref=msg.at[to], dst_ref=recv.at[2 * k + q],
                    send_sem=send, recv_sem=arrive,
                    device_id=(peer, to), device_id_type=MESH,
                )
            )
    for copy in copies:
        copy.start()

    first = vals[:, :half]
    second = pltpu.roll(vals[...], shift, 1)[:, :half]
    sbuf[...] = jnp.where(left, second, first)
    v_copy = pltpu.make_async_remote_copy(
        src_ref=sbuf, dst_ref=bv_out.at[pl.ds(mine, own)], send_sem=s_v.at[0], recv_sem=s_v.at[1],
        device_id=(me, 1 - h), device_id_type=MESH,
    )
    v_copy.start()
    bv_out[pl.ds(mine, own), :] = jnp.where(left, first, second)
    others = recv.at[pl.ds(1, 2 * nb - 1)]
    pltpu.make_async_copy(others, others, send).wait()
    pltpu.make_async_copy(others, others, arrive).wait()
    total = msg[h]
    for k in range(1, 2 * nb):
        total = total + recv[k]
    hv_out[...] = (total[:, :half] * scale).reshape(half)
    num_all = jnp.sum(jnp.where(spot == wide - 2, total, 0.0), axis=1, keepdims=True)
    den_all = jnp.sum(jnp.where(spot == wide - 1, total, 0.0), axis=1, keepdims=True)
    ex_out[...] = num_all / den_all
    v_copy.wait()


def solution(mesh):
    nb = mesh.shape["board"]

    def local(opp_reach, hand_rank, hand_cards, pot, bet_frac, trav_reach):
        boards, half = opp_reach.shape
        hands = hand_rank.shape[1]
        own = boards // 2
        hp = up(hands, LANES)
        wide = up(half + 2, LANES)
        rows = up(PAIRS, 4) * 32
        tall = (2 * (PAIRS // 4) + 1) * LANES
        vm = pltpu.VMEM
        dma = pltpu.SemaphoreType.DMA
        value, hand_values, ratio = pl.pallas_call(
            functools.partial(kernel, nb),
            out_shape=(vm((boards, half), F32), vm((half,), F32), vm((1, 1), F32)),
            in_specs=[pl.BlockSpec(memory_space=pl.ANY)] * 6,
            scratch_shapes=[
                vm((2, hands), I32),
                vm((own, hands), I32),
                vm((own, half), BF16),
                vm((own, half), BF16),
                vm((own, hp), BF16),
                vm((own, hp), BF16),
                vm((own, hp), BF16),
                vm((half,), F32),
                vm((half,), F32),
                vm((1, boards), F32),
                vm((1, boards), F32),
                vm((2, hp), I32),
                vm((own, hp), I32),
                vm((own, hp), F32),
                vm((1, hp), F32),
                vm((2 * own, LANES), F32),
                vm((64, LANES), I32),
                vm((6, hp), I32),
                vm((16, hp), I32),
                vm((2, rows, LANES), I32),
                vm((tall, LANES), F32),
                vm((tall, LANES), F32),
                vm((tall, LANES), F32),
                vm((tall // BATCH, LANES), F32),
                vm((tall, LANES), F32),
                vm((2, LANES, LANES), F32),
                vm((2, rows, LANES), F32),
                vm((own * DIGIT, LANES), F32),
                vm((own, hp), F32),
                vm((own, hp), F32),
                vm((own, hp), F32),
                vm((own, hp), I32),
                vm((own, hp), I32),
                vm((own, LANES), F32),
                vm((own, LANES), F32),
                vm((own, hp), F32),
                vm((own, hp), F32),
                vm((own, hp), F32),
                vm((own, hp), F32),
                vm((2, hp), F32),
                vm((own, half), F32),
                vm((2, 1, wide), F32),
                vm((2 * nb, 1, wide), F32),
                dma((7,)),
                dma((2,)),
                dma((2,)),
                dma((2,)),
                dma,
                dma,
            ],
            compiler_params=pltpu.CompilerParams(collective_id=0, has_side_effects=True),
            name="main",
        )(opp_reach, hand_rank, hand_cards.T, pot[None, :], bet_frac[None, :], trav_reach)
        return value, hand_values, ratio[0, 0]

    placed = (P("board", "hand"), P("board", None), P(), P("board"), P("board"), P("hand"))
    return jax.shard_map(
        local,
        mesh=mesh,
        in_specs=placed,
        out_specs=(P("board", "hand"), P("hand"), P()),
        check_vma=False,
    )
```

```python
import functools

import jax
import jax.numpy as jnp
from jax import lax
from jax.experimental import pallas as pl
from jax.experimental.pallas import tpu as pltpu
from jax.sharding import PartitionSpec as P

CARDS = 52
LANES = 128
SLOT = 64
EACH = CARDS - 1
FOLD = CARDS // 2
PAIRS = FOLD // 2
ROWS = 56
BATCH = 8
MIDDLE = 662.0
LAG = 4
PARTS = ((0, 2), (2, 4), (4, 7))
FIRST = 8
LEAD = 3
FAR = 1e30
DIGIT = 32
TOPS = 42
UNIT = 8192.0
WBITS = 14
RBITS = 11
MESH = pl.DeviceIdType.MESH
F32 = jnp.float32
BF16 = jnp.bfloat16
I32 = jnp.int32
NT = (((1,), (1,)), ((), ()))


def up(n, m):
    return (n + m - 1) // m * m


def iota(shape, axis, dtype=I32):
    return lax.broadcasted_iota(I32, shape, axis).astype(dtype)


def lookup(table, at):
    return jnp.take_along_axis(table, at, axis=1, mode="promise_in_bounds")


def place(ref, half_ref, left):
    half = half_ref.shape[1]
    ref[...] = jnp.zeros(ref.shape, ref.dtype)
    ref[:, :half] = half_ref[...]
    flat = ref[...].astype(F32)
    ref[...] = jnp.where(left, flat, pltpu.roll(flat, half, 1)).astype(ref.dtype)


def spread(row, rows=8):
    return jnp.broadcast_to(row, (rows, row.shape[1]))


def column(row):
    n = row.shape[1]
    diag = iota((n, n), 0) == iota((n, n), 1)
    return jnp.sum(jnp.where(diag, row, 0.0), axis=1, keepdims=True)


def split3(x):
    top = x.astype(BF16)
    rest = x - top.astype(F32)
    mid = rest.astype(BF16)
    return top, mid, (rest - mid.astype(F32)).astype(BF16)


def join(ref, left, first, second):
    half = first.shape[1]
    ref[...] = jnp.zeros(ref.shape, F32)
    ref[:, :half] = jnp.where(left, second, first)
    back = pltpu.roll(ref[...], half, 1)
    ref[...] = jnp.zeros(ref.shape, F32)
    ref[:, :half] = jnp.where(left, first, second)
    ref[...] = ref[...] + back


def folded(u, v):
    low = u < FOLD
    row_x, slot_x = jnp.where(low, u, EACH - u), jnp.where(low, v - u - 1, v - 1)
    low = v < FOLD
    row_y, slot_y = jnp.where(low, v, EACH - v), jnp.where(low, u + EACH - v, u)
    return (row_x >> 1, SLOT * (row_x & 1) + slot_x), (row_y >> 1, SLOT * (row_y & 1) + slot_y)


def gathered(src, pat, k, groups, width, after=lambda at: at):
    top, low = spread(pat[k : k + 1, :]), after(spread(pat[32 + k : 33 + k, :]))
    accs = [jnp.zeros((8, LANES), I32) for _ in range(groups)]
    for s in range(width // LANES):
        here = top == s
        for g in range(groups):
            piece = src[8 * g : 8 * g + 8, s * LANES : (s + 1) * LANES]
            accs[g] = jnp.where(here, lookup(piece, low), accs[g])
    return accs


def first_part(j, rows):
    quad = iota((rows, LANES), 0) >> 5
    lane = iota((rows, LANES), 1)
    row = 8 * j + 2 * quad + (lane >> 6)
    return (lane & (SLOT - 1)) < EACH - row


def kernel(
    nb, opp, rank, cards, pot, bet, trav, bv_out, hv_out, ex_out,
    cards_s, rank_s, opp_s, opp_t, home, away, got, tra, trb, pots, bets, uv, rk, wf, trf, scal, pat, fold, r2, xy,
    tt, up_t, dn_t, ts, st, sb, sx, c1, ft, hib, lob, eqs, ptop, plow, ct, whole, stake, corr, pk, vals, parts, sbuf, msg, recv,
    sem, s_x, s_t, s_v, send, arrive,
):
    me, h = lax.axis_index("board"), lax.axis_index("hand")
    boards, half = opp.shape
    hands = rank.shape[1]
    own = boards // 2
    hp = wf.shape[1]
    wide = msg.shape[2]
    groups = own // 8
    mine = pl.multiple_of(h * own, own)
    theirs = pl.multiple_of((1 - h) * own, own)
    partner = (me, 1 - h)
    left = h == 0
    loads = [
        pltpu.make_async_copy(cards, cards_s, sem.at[0]),
        pltpu.make_async_copy(rank.at[pl.ds(mine, own)], rank_s, sem.at[1]),
        pltpu.make_async_copy(opp.at[pl.ds(theirs, own)], opp_t, sem.at[2]),
        pltpu.make_async_copy(trav, tra, sem.at[3]),
        pltpu.make_async_copy(pot, pots, sem.at[4]),
        pltpu.make_async_copy(bet, bets, sem.at[5]),
        pltpu.make_async_copy(opp.at[pl.ds(mine, own)], opp_s, sem.at[6]),
    ]
    for copy in loads:
        copy.start()
    barrier = pltpu.get_barrier_semaphore()
    for k in range(nb):
        peer = lax.rem(me + k, nb)
        if k:
            pl.semaphore_signal(barrier, inc=1, device_id=(peer, h), device_id_type=MESH)
        pl.semaphore_signal(barrier, inc=1, device_id=(peer, 1 - h), device_id_type=MESH)
    for copy in loads:
        copy.wait()
    place(away, opp_t, left)
    pl.semaphore_wait(barrier, 2 * nb - 1)
    x_copy = pltpu.make_async_remote_copy(
        src_ref=away, dst_ref=got, send_sem=s_x.at[0], recv_sem=s_x.at[1],
        device_id=partner, device_id_type=MESH,
    )
    x_copy.start()
    t_copy = pltpu.make_async_remote_copy(
        src_ref=tra, dst_ref=trb, send_sem=s_t.at[0], recv_sem=s_t.at[1],
        device_id=partner, device_id_type=MESH,
    )
    t_copy.start()

    uv[...] = jnp.full(uv.shape, -1, I32)
    uv[:, :hands] = cards_s[...]
    u, v = uv[0:1, :], uv[1:2, :]
    lane = iota((1, hp), 1)
    at_top, at_low = (lane // LANES + 1).astype(F32), (lane % LANES).astype(F32)
    pair = iota((16, hp), 0)
    spot = iota((LANES, hp), 0, F32).astype(BF16)
    for q, (prow, plane) in enumerate(folded(u, v)):
        fold[2 * q : 2 * q + 1, :] = prow
        fold[2 * q + 1 : 2 * q + 2, :] = plane
        in_pair = pair == prow
        lhs = jnp.concatenate([jnp.where(in_pair, at_top, 0.0), jnp.where(in_pair, at_low, 0.0)], axis=0)
        rhs = jnp.where(spot == spread(plane.astype(F32).astype(BF16), LANES), jnp.ones((), BF16), jnp.zeros((), BF16))
        index = lax.dot_general(lhs.astype(BF16), rhs, NT, preferred_element_type=F32).astype(I32)
        pat[16 * q : 16 * q + 16, :] = index[0:16] - 1
        pat[32 + 16 * q : 48 + 16 * q, :] = index[16:32]
    fold[4:6, :] = jnp.maximum(uv[...], 0)
    place(home, opp_s, left)
    half_pot = 0.5 * column(pots[...])
    win = half_pot + column(bets[...] * pots[...])
    scal[0:own, :] = jnp.broadcast_to(jnp.where(left, win[0:own], win[own:]) * (1.0 / hands), (own, LANES))
    scal[own:, :] = jnp.broadcast_to(jnp.where(left, half_pot[0:own], half_pot[own:]) * (1.0 / hands), (own, LANES))

    rk[...] = jnp.zeros(rk.shape, I32)
    rk[:, :hands] = rank_s[...]
    r2[...] = rk[0:16, :] + (rk[16:32, :] << RBITS)
    columns = hp // LANES
    full = PAIRS // 4
    rest = slice(full * LANES, full * LANES + 32)
    nhi = up(TOPS, 16)
    steps = up(DIGIT, 3) // 3
    hi_row = iota((nhi, hp), 0, F32).astype(BF16)
    lo_row = iota((DIGIT, hp), 0, F32).astype(BF16)

    def digits(c):
        cols = slice(c * LANES, (c + 1) * LANES)
        r = rk[:, cols]
        lo, hi = r & (DIGIT - 1), r >> 5
        top = (lo * 43) >> 7
        hib[:, cols] = hi.astype(F32)
        lob[:, cols] = lo.astype(F32)
        ptop[:, cols] = top
        plow[:, cols] = (lo - 3 * top) * TOPS + hi

    def stretch(ref, b, rows):
        tile = spread(ref[b : b + 1, :], 16).astype(BF16)
        return jnp.concatenate([tile] * (rows // 16), axis=0)

    def marks(b):
        eq = jnp.where(hi_row == stretch(hib, b, nhi), jnp.ones((), BF16), jnp.zeros((), BF16))
        passed.append(eq[0:16, 0:LANES].astype(F32)[0:8])
        eqs[b] = eq

    def after(at, lag):
        if len(passed) < lag:
            return at
        return jnp.where(passed[-lag] > FAR, 0, at)

    def gather_rank(p, q):
        for g, both in enumerate(gathered(r2, pat, 16 * q + p, 2, hp, make(after, lag=LEAD))):
            row = p * 32 + 8 * g
            xy[q, row : row + 8, :] = (both & ((1 << RBITS) - 1)) << WBITS
            xy[q, row + 16 : row + 24, :] = (both >> RBITS) << WBITS

    def weave(streams):
        most = max(len(x) for x in streams)
        done = [0] * len(streams)
        for i in range(1, most + 1):
            for k, stream in enumerate(streams):
                while done[k] * most < i * len(stream):
                    stream[done[k]]()
                    done[k] += 1

    def run(*streams):
        run_each([streams])

    def run_each(groups_of):
        def body(i, carry):
            passed.clear()
            for streams in groups_of:
                weave(streams)
            passed.clear()
            return carry

        lax.fori_loop(0, once, body, 0)

    passed = []
    once = 1 + me // nb
    make = functools.partial
    weave([[make(digits, c) for c in range(columns)]])
    run([make(gather_rank, p, q) for p in range(PAIRS) for q in range(2)], [make(marks, b) for b in range(own)])
    t_copy.wait()
    x_copy.wait()
    wf[...] = home[...].astype(F32) + got[...].astype(F32)
    wi = (wf[...] * UNIT).astype(I32)
    r2[...] = wi[0:16] + (wi[16:32] << WBITS)

    def gather(p, q):
        for g, both in enumerate(gathered(r2, pat, 16 * q + p, 2, hp, make(after, lag=LAG))):
            row = p * 32 + 8 * g
            xy[q, row : row + 8, :] = xy[q, row : row + 8, :] + (both & ((1 << WBITS) - 1))
            xy[q, row + 16 : row + 24, :] = xy[q, row + 16 : row + 24, :] + (both >> WBITS)

    def load_rows(n, packed):
        rows = slice(n * LANES, (n + 1) * LANES)
        both = packed.T
        t = (both >> WBITS).astype(F32) - MIDDLE
        w = (both & ((1 << WBITS) - 1)).astype(F32) * (1.0 / UNIT)
        tt[rows, :] = t
        up_t[rows, :] = t + w
        dn_t[rows, :] = t - w
        slot = iota((LANES, LANES), 0) & (SLOT - 1)
        sums = jnp.sum(jnp.where(slot < EACH, t, 0.0).reshape(LANES // BATCH, BATCH, LANES), axis=1)
        ts[n * (LANES // BATCH) : (n + 1) * (LANES // BATCH), :] = sums

    def load_block(j, side):
        if j < full:
            rows = slice(j * LANES, (j + 1) * LANES)
            part = first_part(j, LANES)
            load_rows(2 * j + side, jnp.where(part, xy[side, rows, :], xy[1 - side, rows, :]))
        else:
            part = first_part(full, 32)
            x, y = xy[0, rest, :], xy[1, rest, :]
            lo_r, hi_r = jnp.where(part, x, y), jnp.where(part, y, x)
            load_rows(2 * full, jnp.concatenate([lo_r, pltpu.roll(lo_r, SLOT, 1), hi_r, pltpu.roll(hi_r, SLOT, 1)], axis=0))

    def pair_tasks(n):
        base = n * SLOT
        state = []

        def step(d0, d1, e0):
            mine_rows = slice(base + 8 * d0, base + 8 * d1)
            here = tt[mine_rows, :]
            size = min(BATCH, EACH - e0)
            at = (base + e0) // BATCH
            some = None
            for e in range(base + e0, base + e0 + size):
                piece = jnp.minimum(jnp.maximum(here, dn_t[e : e + 1, :]), up_t[e : e + 1, :])
                some = piece - ts[at : at + 1, :] if some is None else some + piece
            passed.append(some[0:8])
            acc = state.pop() + some if e0 else some
            if e0 + size == EACH:
                st[mine_rows, :] = acc
                if d0 == 0:
                    st[base + ROWS : base + SLOT, :] = jnp.zeros((SLOT - ROWS, LANES), F32)
            else:
                state.append(acc)

        return [make(step, d0, d1, e0) for d0, d1 in PARTS for e0 in range(0, EACH, BATCH)]

    def hist(b):
        lw = jnp.where(stretch(lob, b, DIGIT) <= lo_row, stretch(wf, b, DIGIT), jnp.zeros((), BF16))
        if b < FIRST:
            passed.append(lw[0:16, 0:LANES].astype(F32)[0:8])
        c1[b * DIGIT : (b + 1) * DIGIT, 0:nhi] = lax.dot_general(lw, eqs[b], NT, preferred_element_type=F32)

    lanes = iota((8, LANES), 1)
    a, z = iota((LANES, LANES), 0), iota((LANES, LANES), 1)
    sgn = jnp.where(z > a, 1, jnp.where(z < a, -1, 0)).astype(F32).astype(BF16)

    def table(g):
        sums = jnp.where(lanes < TOPS, c1[pl.ds(g * 8 * DIGIT + DIGIT - 1, 8, stride=DIGIT), :], 0.0)
        base = -sums
        for piece in split3(sums):
            base = base + jnp.dot(piece, sgn, preferred_element_type=F32)
        below = jnp.zeros((8, LANES), F32)
        row = []
        for lo in range(DIGIT):
            upto = c1[pl.ds(g * 8 * DIGIT + lo, 8, stride=DIGIT), :]
            row.append(base + (below + upto))
            below = upto
        for s in range(steps):
            out = row[3 * s]
            for q in range(1, 3):
                if 3 * s + q < DIGIT:
                    out = jnp.where(lanes < q * TOPS, out, pltpu.roll(row[3 * s + q], q * TOPS, 1))
            ft[8 * g : 8 * g + 8, s * LANES : (s + 1) * LANES] = out

    def pick(g, c):
        rows, cols = slice(8 * g, 8 * g + 8), slice(c * LANES, (c + 1) * LANES)
        top, low = ptop[rows, cols], after(plow[rows, cols], LAG)
        out = jnp.zeros((8, LANES), F32)
        for s in range(steps):
            out = jnp.where(top == s, lookup(ft[rows, s * LANES : (s + 1) * LANES], low), out)
        pk[rows, cols] = out

    def totals():
        card_row = iota((LANES, hp), 0)
        hold = ((card_row == uv[0:1, :]) | (card_row == uv[1:2, :])).astype(F32).astype(BF16)
        taken = lax.dot_general(wf[...].astype(BF16), hold, NT, preferred_element_type=F32)
        ct[...] = taken
        whole[...] = jnp.broadcast_to(0.5 * jnp.sum(taken, axis=1, keepdims=True), (own, LANES))

    def stakes(c):
        cols = slice(c * LANES, (c + 1) * LANES)
        ua, va = spread(fold[4:5, cols]), spread(fold[5:6, cols])
        for g in range(groups):
            rows = slice(8 * g, 8 * g + 8)
            t = ct[rows, :]
            live = whole[rows, :] - lookup(t, ua) - lookup(t, va) + wf[rows, cols]
            stake[rows, cols] = scal[own + 8 * g : own + 8 * g + 8, :] * live

    def back(j, side):
        if j < full:
            rows = slice((2 * j + side) * LANES, (2 * j + side + 1) * LANES)
            sb[side] = st[rows, :].T
            if side:
                out = slice(j * LANES, (j + 1) * LANES)
                part = first_part(j, LANES)
                sx[0, out, :] = jnp.where(part, sb[0], sb[1])
                sx[1, out, :] = jnp.where(part, sb[1], sb[0])
        else:
            last = st[2 * full * LANES : (2 * full + 1) * LANES, :].T
            at_left = iota((32, LANES), 1) < SLOT
            lo_r = jnp.where(at_left, last[0:32], pltpu.roll(last[32:64], SLOT, 1))
            hi_r = jnp.where(at_left, last[64:96], pltpu.roll(last[96:128], SLOT, 1))
            part = first_part(full, 32)
            sx[0, rest, :] = jnp.where(part, lo_r, hi_r)
            sx[1, rest, :] = jnp.where(part, hi_r, lo_r)

    def scatter(j, c, stop):
        cols = slice(c * LANES, (c + 1) * LANES)
        out = [None] * groups
        for q in range(2):
            top, low = spread(fold[2 * q : 2 * q + 1, cols]), after(spread(fold[2 * q + 1 : 2 * q + 2, cols]), LAG)
            accs = [jnp.zeros((8, LANES), F32) for _ in range(groups)]
            for p in range(4 * j, stop):
                here = top == p
                for g in range(groups):
                    accs[g] = jnp.where(here, lookup(sx[q, p * 32 + 8 * g : p * 32 + 8 * g + 8, :], low), accs[g])
            out = [y if x is None else x + y for x, y in zip(out, accs)]
        return out

    def scatter_add(j, c):
        cols = slice(c * LANES, (c + 1) * LANES)
        for g, x in enumerate(scatter(j, c, 4 * j + 4)):
            rows = slice(8 * g, 8 * g + 8)
            corr[rows, cols] = x if j == 0 else corr[rows, cols] + x

    def finish(c):
        cols = slice(c * LANES, (c + 1) * LANES)
        part = jnp.zeros((8, LANES), F32)
        mass = jnp.zeros((8, LANES), F32)
        for g, x in enumerate(scatter(full - 1, c, PAIRS)):
            rows = slice(8 * g, 8 * g + 8)
            margin = pk[rows, cols] - (corr[rows, cols] + x)
            held = stake[rows, cols]
            value = jnp.maximum(scal[rows, :] * margin, -held)
            vals[rows, cols] = value
            part = part + value
            mass = mass + held
        parts[0:1, cols] = jnp.sum(part, axis=0, keepdims=True)
        parts[1:2, cols] = jnp.sum(mass, axis=0, keepdims=True)

    gathers = lambda j: [make(gather, p, q) for p in range(4 * j, min(4 * j + 4, PAIRS)) for q in range(2)]
    loads_of = lambda j: [make(load_block, j, side) for side in range(2 if j < full else 1)]
    pairs = lambda j: [t for n in range(4 * j, 4 * j + (4 if j < full else 1)) for t in pair_tasks(n)]
    backs = lambda j: [make(back, j, side) for side in range(2 if j < full else 1)]
    hists = lambda g: [make(hist, b) for b in range(8 * g, 8 * g + 8)]
    picks = lambda g: [make(table, g)] + [make(pick, g, c) for c in range(columns)]
    adds = lambda j: [make(scatter_add, j, c) for c in range(columns)]

    bins = [make(hist, b) for b in range(own)]
    reads = [t for g in range(groups) for t in picks(g)]
    run([totals] + gathers(0) + loads_of(0), bins[:FIRST])
    held = [make(stakes, c) for c in range(columns)]
    later = gathers(2) + gathers(3)
    add0, add1 = adds(0), adds(1)
    moves = [
        gathers(1)[:4],
        gathers(1)[4:],
        loads_of(1) + later[:4],
        later[4:8],
        backs(0) + later[8:],
        loads_of(2) + add0[:3],
        loads_of(3) + add0[3:6],
        add0[6:9],
        backs(1) + add0[9:],
        add1[:3],
        add1[3:6],
        add1[6:9],
        backs(2) + add1[9:],
    ]
    more = [8, 11, 14, 17, 20, 22, 24, 27, 30, 32, 32, 32, 32, 32]
    look = [0, 1, 4, 7, 12, 13, 17, 21, 25, 29, 33, 37, 42, 48]
    for span in (range(0, 4), range(4, 8), range(8, 12), range(12, 13)):
        run_each([(moves[k] + reads[look[k] : look[k + 1]] + held[k : k + 1], pair_tasks(k), bins[more[k] : more[k + 1]]) for k in span])
    run(backs(3), [make(finish, c) for c in range(columns)])
    join(trf, left, tra[...].reshape(1, half), trb[...].reshape(1, half))

    scale = 1.0 / (boards * nb)
    shift = hp - half
    trow = trf[...]
    num = jnp.sum(trow * parts[0:1, :], axis=1, keepdims=True)
    den = jnp.sum(trow * parts[1:2, :], axis=1, keepdims=True)
    spot = iota((1, wide), 1)
    tail = jnp.where(spot == wide - 2, num, jnp.where(spot == wide - 1, den, 0.0))
    both = parts[...]
    msg[0] = jnp.where(spot < half, both[0:1, :wide], tail)
    msg[1] = jnp.where(spot < half, pltpu.roll(both, shift, 1)[0:1, :wide], tail)

    copies = []
    for k in range(nb):
        peer = lax.rem(me + k, nb)
        for q in range(2):
            if k == 0 and q == 0:
                continue
            to = h if q == 0 else 1 - h
            copies.append(
                pltpu.make_async_remote_copy(
                    src_ref=msg.at[to], dst_ref=recv.at[2 * k + q],
                    send_sem=send, recv_sem=arrive,
                    device_id=(peer, to), device_id_type=MESH,
                )
            )
    for copy in copies:
        copy.start()

    first = vals[:, :half]
    second = pltpu.roll(vals[...], shift, 1)[:, :half]
    sbuf[...] = jnp.where(left, second, first)
    v_copy = pltpu.make_async_remote_copy(
        src_ref=sbuf, dst_ref=bv_out.at[pl.ds(mine, own)], send_sem=s_v.at[0], recv_sem=s_v.at[1],
        device_id=(me, 1 - h), device_id_type=MESH,
    )
    v_copy.start()
    bv_out[pl.ds(mine, own), :] = jnp.where(left, first, second)
    others = recv.at[pl.ds(1, 2 * nb - 1)]
    pltpu.make_async_copy(others, others, send).wait()
    pltpu.make_async_copy(others, others, arrive).wait()
    total = msg[h]
    for k in range(1, 2 * nb):
        total = total + recv[k]
    hv_out[...] = (total[:, :half] * scale).reshape(half)
    num_all = jnp.sum(jnp.where(spot == wide - 2, total, 0.0), axis=1, keepdims=True)
    den_all = jnp.sum(jnp.where(spot == wide - 1, total, 0.0), axis=1, keepdims=True)
    ex_out[...] = num_all / den_all
    v_copy.wait()


def flush(value, hands, value_out, hands_out, sem):
    pairs = ((value, value_out), (hands, hands_out))
    copies = [pltpu.make_async_copy(a, b, sem.at[k]) for k, (a, b) in enumerate(pairs)]
    for copy in copies:
        copy.start()
    for copy in copies:
        copy.wait()


def solution(mesh):
    nb = mesh.shape["board"]

    def local(opp_reach, hand_rank, hand_cards, pot, bet_frac, trav_reach):
        boards, half = opp_reach.shape
        hands = hand_rank.shape[1]
        own = boards // 2
        hp = up(hands, LANES)
        wide = up(half + 2, LANES)
        rows = up(PAIRS, 4) * 32
        tall = (2 * (PAIRS // 4) + 1) * LANES
        vm = pltpu.VMEM
        dma = pltpu.SemaphoreType.DMA
        value, hand_values, ratio = pl.pallas_call(
            functools.partial(kernel, nb),
            out_shape=(vm((boards, half), F32), vm((half,), F32), vm((1, 1), F32)),
            in_specs=[pl.BlockSpec(memory_space=pl.ANY)] * 6,
            scratch_shapes=[
                vm((2, hands), I32),
                vm((own, hands), I32),
                vm((own, half), BF16),
                vm((own, half), BF16),
                vm((own, hp), BF16),
                vm((own, hp), BF16),
                vm((own, hp), BF16),
                vm((half,), F32),
                vm((half,), F32),
                vm((1, boards), F32),
                vm((1, boards), F32),
                vm((2, hp), I32),
                vm((own, hp), I32),
                vm((own, hp), F32),
                vm((1, hp), F32),
                vm((2 * own, LANES), F32),
                vm((64, LANES), I32),
                vm((6, hp), I32),
                vm((16, hp), I32),
                vm((2, rows, LANES), I32),
                vm((tall, LANES), F32),
                vm((tall, LANES), F32),
                vm((tall, LANES), F32),
                vm((tall // BATCH, LANES), F32),
                vm((tall, LANES), F32),
                vm((2, LANES, LANES), F32),
                vm((2, rows, LANES), F32),
                vm((own * DIGIT, LANES), F32),
                vm((own, hp), F32),
                vm((own, hp), F32),
                vm((own, hp), F32),
                vm((own, up(TOPS, 16), hp), BF16),
                vm((own, hp), I32),
                vm((own, hp), I32),
                vm((own, LANES), F32),
                vm((own, LANES), F32),
                vm((own, hp), F32),
                vm((own, hp), F32),
                vm((own, hp), F32),
                vm((own, hp), F32),
                vm((2, hp), F32),
                vm((own, half), F32),
                vm((2, 1, wide), F32),
                vm((2 * nb, 1, wide), F32),
                dma((7,)),
                dma((2,)),
                dma((2,)),
                dma((2,)),
                dma,
                dma,
            ],
            compiler_params=pltpu.CompilerParams(collective_id=0, has_side_effects=True),
            name="main",
        )(opp_reach, hand_rank, hand_cards.T, pot[None, :], bet_frac[None, :], trav_reach)
        spot = pl.BlockSpec(memory_space=pl.ANY)
        value, hand_values = pl.pallas_call(
            flush,
            out_shape=tuple(jax.ShapeDtypeStruct(x.shape, x.dtype) for x in (value, hand_values)),
            in_specs=[spot] * 2,
            out_specs=[spot] * 2,
            scratch_shapes=[dma((2,))],
            name="flush",
        )(*(pltpu.with_memory_space_constraint(x, pltpu.VMEM) for x in (value, hand_values)))
        return value, hand_values, ratio[0, 0]

    placed = (P("board", "hand"), P("board", None), P(), P("board"), P("board"), P("hand"))
    return jax.shard_map(
        local,
        mesh=mesh,
        in_specs=placed,
        out_specs=(P("board", "hand"), P("hand"), P()),
        check_vma=False,
    )
```

```python
import functools

import jax
import jax.numpy as jnp
from jax import lax
from jax.experimental import pallas as pl
from jax.experimental.pallas import tpu as pltpu
from jax.sharding import PartitionSpec as P

CARDS = 52
LANES = 128
SLOT = 64
EACH = CARDS - 1
FOLD = CARDS // 2
PAIRS = FOLD // 2
ROWS = 56
BATCH = 8
MIDDLE = 662.0
LAG = 4
PARTS = ((0, 2), (2, 4), (4, 7))
FIRST = 6
LEAD = 3
EARLY = 8
FAR = 1e30
DIGIT = 32
TOPS = 42
UNIT = 8192.0
WBITS = 14
RBITS = 11
MESH = pl.DeviceIdType.MESH
F32 = jnp.float32
BF16 = jnp.bfloat16
I32 = jnp.int32
NT = (((1,), (1,)), ((), ()))


def up(n, m):
    return (n + m - 1) // m * m


def iota(shape, axis, dtype=I32):
    return lax.broadcasted_iota(I32, shape, axis).astype(dtype)


def lookup(table, at):
    return jnp.take_along_axis(table, at, axis=1, mode="promise_in_bounds")


def place(ref, half_ref, left):
    half = half_ref.shape[1]
    ref[...] = jnp.zeros(ref.shape, ref.dtype)
    ref[:, :half] = half_ref[...]
    flat = ref[...].astype(F32)
    ref[...] = jnp.where(left, flat, pltpu.roll(flat, half, 1)).astype(ref.dtype)


def spread(row, rows=8):
    return jnp.broadcast_to(row, (rows, row.shape[1]))


def column(row):
    n = row.shape[1]
    diag = iota((n, n), 0) == iota((n, n), 1)
    return jnp.sum(jnp.where(diag, row, 0.0), axis=1, keepdims=True)


def split3(x):
    top = x.astype(BF16)
    rest = x - top.astype(F32)
    mid = rest.astype(BF16)
    return top, mid, (rest - mid.astype(F32)).astype(BF16)


def join(ref, left, first, second):
    half = first.shape[1]
    ref[...] = jnp.zeros(ref.shape, F32)
    ref[:, :half] = jnp.where(left, second, first)
    back = pltpu.roll(ref[...], half, 1)
    ref[...] = jnp.zeros(ref.shape, F32)
    ref[:, :half] = jnp.where(left, first, second)
    ref[...] = ref[...] + back


def folded(u, v):
    low = u < FOLD
    row_x, slot_x = jnp.where(low, u, EACH - u), jnp.where(low, v - u - 1, v - 1)
    low = v < FOLD
    row_y, slot_y = jnp.where(low, v, EACH - v), jnp.where(low, u + EACH - v, u)
    return (row_x >> 1, SLOT * (row_x & 1) + slot_x), (row_y >> 1, SLOT * (row_y & 1) + slot_y)


def gathered(src, pat, k, groups, width, after=lambda at: at):
    top, low = spread(pat[k : k + 1, :]), after(spread(pat[32 + k : 33 + k, :]))
    accs = [jnp.zeros((8, LANES), I32) for _ in range(groups)]
    for s in range(width // LANES):
        here = top == s
        for g in range(groups):
            piece = src[8 * g : 8 * g + 8, s * LANES : (s + 1) * LANES]
            accs[g] = jnp.where(here, lookup(piece, low), accs[g])
    return accs


def first_part(j, rows):
    quad = iota((rows, LANES), 0) >> 5
    lane = iota((rows, LANES), 1)
    row = 8 * j + 2 * quad + (lane >> 6)
    return (lane & (SLOT - 1)) < EACH - row


def kernel(
    nb, opp, rank, cards, pot, bet, trav, bv_out, hv_out, ex_out,
    cards_s, rank_s, opp_s, opp_t, home, away, got, tra, trb, pots, bets, uv, rk, wf, trf, scal, pat, fold, r2, xy,
    tt, up_t, dn_t, ts, st, sb, sx, c1, ft, hib, lob, eqs, ptop, plow, ct, whole, stake, corr, pk, vals, parts, sbuf, msg, recv,
    sem, s_x, s_t, s_v, send, arrive,
):
    me, h = lax.axis_index("board"), lax.axis_index("hand")
    boards, half = opp.shape
    hands = rank.shape[1]
    own = boards // 2
    hp = wf.shape[1]
    wide = msg.shape[2]
    groups = own // 8
    mine = pl.multiple_of(h * own, own)
    theirs = pl.multiple_of((1 - h) * own, own)
    partner = (me, 1 - h)
    left = h == 0
    loads = [
        pltpu.make_async_copy(cards, cards_s, sem.at[0]),
        pltpu.make_async_copy(rank.at[pl.ds(mine, own)], rank_s, sem.at[1]),
        pltpu.make_async_copy(opp.at[pl.ds(theirs, own)], opp_t, sem.at[2]),
        pltpu.make_async_copy(trav, tra, sem.at[3]),
        pltpu.make_async_copy(pot, pots, sem.at[4]),
        pltpu.make_async_copy(bet, bets, sem.at[5]),
        pltpu.make_async_copy(opp.at[pl.ds(mine, own)], opp_s, sem.at[6]),
    ]
    for copy in loads:
        copy.start()
    barrier = pltpu.get_barrier_semaphore()
    for k in range(nb):
        peer = lax.rem(me + k, nb)
        if k:
            pl.semaphore_signal(barrier, inc=1, device_id=(peer, h), device_id_type=MESH)
        pl.semaphore_signal(barrier, inc=1, device_id=(peer, 1 - h), device_id_type=MESH)
    for copy in loads:
        copy.wait()
    place(away, opp_t, left)
    pl.semaphore_wait(barrier, 2 * nb - 1)
    x_copy = pltpu.make_async_remote_copy(
        src_ref=away, dst_ref=got, send_sem=s_x.at[0], recv_sem=s_x.at[1],
        device_id=partner, device_id_type=MESH,
    )
    x_copy.start()
    t_copy = pltpu.make_async_remote_copy(
        src_ref=tra, dst_ref=trb, send_sem=s_t.at[0], recv_sem=s_t.at[1],
        device_id=partner, device_id_type=MESH,
    )
    t_copy.start()

    uv[...] = jnp.full(uv.shape, -1, I32)
    uv[:, :hands] = cards_s[...]
    u, v = uv[0:1, :], uv[1:2, :]
    lane = iota((1, hp), 1)
    at_top, at_low = (lane // LANES + 1).astype(F32), (lane % LANES).astype(F32)
    pair = iota((16, hp), 0)
    spot = iota((LANES, hp), 0, F32).astype(BF16)
    for q, (prow, plane) in enumerate(folded(u, v)):
        fold[2 * q : 2 * q + 1, :] = prow
        fold[2 * q + 1 : 2 * q + 2, :] = plane
        in_pair = pair == prow
        lhs = jnp.concatenate([jnp.where(in_pair, at_top, 0.0), jnp.where(in_pair, at_low, 0.0)], axis=0)
        rhs = jnp.where(spot == spread(plane.astype(F32).astype(BF16), LANES), jnp.ones((), BF16), jnp.zeros((), BF16))
        index = lax.dot_general(lhs.astype(BF16), rhs, NT, preferred_element_type=F32).astype(I32)
        pat[16 * q : 16 * q + 16, :] = index[0:16] - 1
        pat[32 + 16 * q : 48 + 16 * q, :] = index[16:32]
    fold[4:6, :] = jnp.maximum(uv[...], 0)
    place(home, opp_s, left)
    half_pot = 0.5 * column(pots[...])
    win = half_pot + column(bets[...] * pots[...])
    scal[0:own, :] = jnp.broadcast_to(jnp.where(left, win[0:own], win[own:]) * (1.0 / hands), (own, LANES))
    scal[own:, :] = jnp.broadcast_to(jnp.where(left, half_pot[0:own], half_pot[own:]) * (1.0 / hands), (own, LANES))

    rk[...] = jnp.zeros(rk.shape, I32)
    rk[:, :hands] = rank_s[...]
    r2[...] = rk[0:16, :] + (rk[16:32, :] << RBITS)
    columns = hp // LANES
    full = PAIRS // 4
    rest = slice(full * LANES, full * LANES + 32)
    nhi = up(TOPS, 16)
    steps = up(DIGIT, 3) // 3
    hi_row = iota((nhi, hp), 0, F32).astype(BF16)
    lo_row = iota((DIGIT, hp), 0, F32).astype(BF16)

    def digits(c):
        cols = slice(c * LANES, (c + 1) * LANES)
        r = rk[:, cols]
        lo, hi = r & (DIGIT - 1), r >> 5
        top = (lo * 43) >> 7
        hib[:, cols] = hi.astype(F32)
        lob[:, cols] = lo.astype(F32)
        ptop[:, cols] = top
        plow[:, cols] = (lo - 3 * top) * TOPS + hi

    def stretch(ref, b, rows):
        tile = spread(ref[b : b + 1, :], 16).astype(BF16)
        return jnp.concatenate([tile] * (rows // 16), axis=0)

    def ones(b):
        return jnp.where(hi_row == stretch(hib, b, nhi), jnp.ones((), BF16), jnp.zeros((), BF16))

    def marks(b):
        eq = ones(b)
        passed.append(eq[0:16, 0:LANES].astype(F32)[0:8])
        eqs[b] = eq

    def after(at, lag):
        if len(passed) < lag:
            return at
        return jnp.where(passed[-lag] > FAR, 0, at)

    def gather_rank(p, q):
        for g, both in enumerate(gathered(r2, pat, 16 * q + p, 2, hp, make(after, lag=LEAD))):
            row = p * 32 + 8 * g
            xy[q, row : row + 8, :] = (both & ((1 << RBITS) - 1)) << WBITS
            xy[q, row + 16 : row + 24, :] = (both >> RBITS) << WBITS

    def weave(streams):
        most = max(len(x) for x in streams)
        done = [0] * len(streams)
        for i in range(1, most + 1):
            for k, stream in enumerate(streams):
                while done[k] * most < i * len(stream):
                    stream[done[k]]()
                    done[k] += 1

    def run(*streams):
        run_each([streams])

    def run_each(groups_of):
        def body(i, carry):
            passed.clear()
            for streams in groups_of:
                weave(streams)
            passed.clear()
            return carry

        lax.fori_loop(0, once, body, 0)

    passed = []
    once = 1 + me // nb
    make = functools.partial
    weave([[make(digits, c) for c in range(columns)]])
    run([make(gather_rank, p, q) for p in range(PAIRS) for q in range(2)], [make(marks, b) for b in range(EARLY, own)])
    t_copy.wait()
    x_copy.wait()
    wf[...] = home[...].astype(F32) + got[...].astype(F32)
    wi = (wf[...] * UNIT).astype(I32)
    r2[...] = wi[0:16] + (wi[16:32] << WBITS)

    def gather(p, q):
        for g, both in enumerate(gathered(r2, pat, 16 * q + p, 2, hp, make(after, lag=LAG))):
            row = p * 32 + 8 * g
            xy[q, row : row + 8, :] = xy[q, row : row + 8, :] + (both & ((1 << WBITS) - 1))
            xy[q, row + 16 : row + 24, :] = xy[q, row + 16 : row + 24, :] + (both >> WBITS)

    def load_rows(n, packed):
        rows = slice(n * LANES, (n + 1) * LANES)
        both = packed.T
        t = (both >> WBITS).astype(F32) - MIDDLE
        w = (both & ((1 << WBITS) - 1)).astype(F32) * (1.0 / UNIT)
        tt[rows, :] = t
        up_t[rows, :] = t + w
        dn_t[rows, :] = t - w
        slot = iota((LANES, LANES), 0) & (SLOT - 1)
        sums = jnp.sum(jnp.where(slot < EACH, t, 0.0).reshape(LANES // BATCH, BATCH, LANES), axis=1)
        ts[n * (LANES // BATCH) : (n + 1) * (LANES // BATCH), :] = sums

    def load_block(j, side):
        if j < full:
            rows = slice(j * LANES, (j + 1) * LANES)
            part = first_part(j, LANES)
            load_rows(2 * j + side, jnp.where(part, xy[side, rows, :], xy[1 - side, rows, :]))
        else:
            part = first_part(full, 32)
            x, y = xy[0, rest, :], xy[1, rest, :]
            lo_r, hi_r = jnp.where(part, x, y), jnp.where(part, y, x)
            load_rows(2 * full, jnp.concatenate([lo_r, pltpu.roll(lo_r, SLOT, 1), hi_r, pltpu.roll(hi_r, SLOT, 1)], axis=0))

    def pair_tasks(n):
        base = n * SLOT
        state = []

        def step(d0, d1, e0):
            mine_rows = slice(base + 8 * d0, base + 8 * d1)
            here = tt[mine_rows, :]
            size = min(BATCH, EACH - e0)
            at = (base + e0) // BATCH
            some = None
            for e in range(base + e0, base + e0 + size):
                piece = jnp.minimum(jnp.maximum(here, dn_t[e : e + 1, :]), up_t[e : e + 1, :])
                some = piece - ts[at : at + 1, :] if some is None else some + piece
            passed.append(some[0:8])
            acc = state.pop() + some if e0 else some
            if e0 + size == EACH:
                st[mine_rows, :] = acc
                if d0 == 0:
                    st[base + ROWS : base + SLOT, :] = jnp.zeros((SLOT - ROWS, LANES), F32)
            else:
                state.append(acc)

        return [make(step, d0, d1, e0) for d0, d1 in PARTS for e0 in range(0, EACH, BATCH)]

    def hist(b):
        lw = jnp.where(stretch(lob, b, DIGIT) <= lo_row, stretch(wf, b, DIGIT), jnp.zeros((), BF16))
        if b < FIRST:
            passed.append(lw[0:16, 0:LANES].astype(F32)[0:8])
        c1[b * DIGIT : (b + 1) * DIGIT, 0:nhi] = lax.dot_general(lw, ones(b) if b < EARLY else eqs[b], NT, preferred_element_type=F32)

    lanes = iota((8, LANES), 1)
    a, z = iota((LANES, LANES), 0), iota((LANES, LANES), 1)
    sgn = jnp.where(z > a, 1, jnp.where(z < a, -1, 0)).astype(F32).astype(BF16)

    def table(g):
        sums = jnp.where(lanes < TOPS, c1[pl.ds(g * 8 * DIGIT + DIGIT - 1, 8, stride=DIGIT), :], 0.0)
        base = -sums
        for piece in split3(sums):
            base = base + jnp.dot(piece, sgn, preferred_element_type=F32)
        below = jnp.zeros((8, LANES), F32)
        row = []
        for lo in range(DIGIT):
            upto = c1[pl.ds(g * 8 * DIGIT + lo, 8, stride=DIGIT), :]
            row.append(base + (below + upto))
            below = upto
        for s in range(steps):
            out = row[3 * s]
            for q in range(1, 3):
                if 3 * s + q < DIGIT:
                    out = jnp.where(lanes < q * TOPS, out, pltpu.roll(row[3 * s + q], q * TOPS, 1))
            ft[8 * g : 8 * g + 8, s * LANES : (s + 1) * LANES] = out

    def pick(g, c):
        rows, cols = slice(8 * g, 8 * g + 8), slice(c * LANES, (c + 1) * LANES)
        top, low = ptop[rows, cols], after(plow[rows, cols], LAG)
        out = jnp.zeros((8, LANES), F32)
        for s in range(steps):
            out = jnp.where(top == s, lookup(ft[rows, s * LANES : (s + 1) * LANES], low), out)
        pk[rows, cols] = out

    def totals():
        card_row = iota((LANES, hp), 0)
        hold = ((card_row == uv[0:1, :]) | (card_row == uv[1:2, :])).astype(F32).astype(BF16)
        taken = lax.dot_general(wf[...].astype(BF16), hold, NT, preferred_element_type=F32)
        ct[...] = taken
        whole[...] = jnp.broadcast_to(0.5 * jnp.sum(taken, axis=1, keepdims=True), (own, LANES))

    def stakes(c):
        cols = slice(c * LANES, (c + 1) * LANES)
        ua, va = spread(fold[4:5, cols]), spread(fold[5:6, cols])
        for g in range(groups):
            rows = slice(8 * g, 8 * g + 8)
            t = ct[rows, :]
            live = whole[rows, :] - lookup(t, ua) - lookup(t, va) + wf[rows, cols]
            stake[rows, cols] = scal[own + 8 * g : own + 8 * g + 8, :] * live

    def back(j, side):
        if j < full:
            rows = slice((2 * j + side) * LANES, (2 * j + side + 1) * LANES)
            sb[side] = st[rows, :].T
            if side:
                out = slice(j * LANES, (j + 1) * LANES)
                part = first_part(j, LANES)
                sx[0, out, :] = jnp.where(part, sb[0], sb[1])
                sx[1, out, :] = jnp.where(part, sb[1], sb[0])
        else:
            last = st[2 * full * LANES : (2 * full + 1) * LANES, :].T
            at_left = iota((32, LANES), 1) < SLOT
            lo_r = jnp.where(at_left, last[0:32], pltpu.roll(last[32:64], SLOT, 1))
            hi_r = jnp.where(at_left, last[64:96], pltpu.roll(last[96:128], SLOT, 1))
            part = first_part(full, 32)
            sx[0, rest, :] = jnp.where(part, lo_r, hi_r)
            sx[1, rest, :] = jnp.where(part, hi_r, lo_r)

    def scatter(j, c, stop):
        cols = slice(c * LANES, (c + 1) * LANES)
        out = [None] * groups
        for q in range(2):
            top, low = spread(fold[2 * q : 2 * q + 1, cols]), after(spread(fold[2 * q + 1 : 2 * q + 2, cols]), LAG)
            accs = [jnp.zeros((8, LANES), F32) for _ in range(groups)]
            for p in range(4 * j, stop):
                here = top == p
                for g in range(groups):
                    accs[g] = jnp.where(here, lookup(sx[q, p * 32 + 8 * g : p * 32 + 8 * g + 8, :], low), accs[g])
            out = [y if x is None else x + y for x, y in zip(out, accs)]
        return out

    def scatter_add(j, c):
        cols = slice(c * LANES, (c + 1) * LANES)
        for g, x in enumerate(scatter(j, c, 4 * j + 4)):
            rows = slice(8 * g, 8 * g + 8)
            corr[rows, cols] = x if j == 0 else corr[rows, cols] + x

    def finish(c):
        cols = slice(c * LANES, (c + 1) * LANES)
        part = jnp.zeros((8, LANES), F32)
        mass = jnp.zeros((8, LANES), F32)
        for g, x in enumerate(scatter(full - 1, c, PAIRS)):
            rows = slice(8 * g, 8 * g + 8)
            margin = pk[rows, cols] - (corr[rows, cols] + x)
            held = stake[rows, cols]
            value = jnp.maximum(scal[rows, :] * margin, -held)
            vals[rows, cols] = value
            part = part + value
            mass = mass + held
        parts[0:1, cols] = jnp.sum(part, axis=0, keepdims=True)
        parts[1:2, cols] = jnp.sum(mass, axis=0, keepdims=True)

    gathers = lambda j: [make(gather, p, q) for p in range(4 * j, min(4 * j + 4, PAIRS)) for q in range(2)]
    loads_of = lambda j: [make(load_block, j, side) for side in range(2 if j < full else 1)]
    pairs = lambda j: [t for n in range(4 * j, 4 * j + (4 if j < full else 1)) for t in pair_tasks(n)]
    backs = lambda j: [make(back, j, side) for side in range(2 if j < full else 1)]
    hists = lambda g: [make(hist, b) for b in range(8 * g, 8 * g + 8)]
    picks = lambda g: [make(table, g)] + [make(pick, g, c) for c in range(columns)]
    adds = lambda j: [make(scatter_add, j, c) for c in range(columns)]

    bins = [make(hist, b) for b in range(own)]
    reads = [t for g in range(groups) for t in picks(g)]
    run([totals] + gathers(0) + loads_of(0), bins[:FIRST])
    held = [make(stakes, c) for c in range(columns)]
    later = gathers(2) + gathers(3)
    add0, add1 = adds(0), adds(1)
    moves = [
        gathers(1)[:4],
        gathers(1)[4:],
        loads_of(1) + later[:4],
        later[4:8],
        backs(0) + later[8:],
        loads_of(2) + add0[:3],
        loads_of(3) + add0[3:6],
        add0[6:9],
        backs(1) + add0[9:],
        add1[:3],
        add1[3:6],
        add1[6:9],
        backs(2) + add1[9:],
    ]
    more = [6, 9, 12, 15, 18, 20, 22, 25, 28, 30, 32, 32, 32, 32]
    look = [0, 0, 4, 8, 12, 13, 17, 21, 25, 29, 33, 37, 42, 48]
    for span in (range(0, 4), range(4, 8), range(8, 12), range(12, 13)):
        run_each([(moves[k] + reads[look[k] : look[k + 1]] + held[k : k + 1], pair_tasks(k), bins[more[k] : more[k + 1]]) for k in span])
    run(backs(3), [make(finish, c) for c in range(columns)])
    join(trf, left, tra[...].reshape(1, half), trb[...].reshape(1, half))

    scale = 1.0 / (boards * nb)
    shift = hp - half
    trow = trf[...]
    num = jnp.sum(trow * parts[0:1, :], axis=1, keepdims=True)
    den = jnp.sum(trow * parts[1:2, :], axis=1, keepdims=True)
    spot = iota((1, wide), 1)
    tail = jnp.where(spot == wide - 2, num, jnp.where(spot == wide - 1, den, 0.0))
    both = parts[...]
    msg[0] = jnp.where(spot < half, both[0:1, :wide], tail)
    msg[1] = jnp.where(spot < half, pltpu.roll(both, shift, 1)[0:1, :wide], tail)

    copies = []
    for k in range(nb):
        peer = lax.rem(me + k, nb)
        for q in range(2):
            if k == 0 and q == 0:
                continue
            to = h if q == 0 else 1 - h
            copies.append(
                pltpu.make_async_remote_copy(
                    src_ref=msg.at[to], dst_ref=recv.at[2 * k + q],
                    send_sem=send, recv_sem=arrive,
                    device_id=(peer, to), device_id_type=MESH,
                )
            )
    for copy in copies:
        copy.start()

    first = vals[:, :half]
    second = pltpu.roll(vals[...], shift, 1)[:, :half]
    sbuf[...] = jnp.where(left, second, first)
    v_copy = pltpu.make_async_remote_copy(
        src_ref=sbuf, dst_ref=bv_out.at[pl.ds(mine, own)], send_sem=s_v.at[0], recv_sem=s_v.at[1],
        device_id=(me, 1 - h), device_id_type=MESH,
    )
    v_copy.start()
    bv_out[pl.ds(mine, own), :] = jnp.where(left, first, second)
    others = recv.at[pl.ds(1, 2 * nb - 1)]
    pltpu.make_async_copy(others, others, send).wait()
    pltpu.make_async_copy(others, others, arrive).wait()
    total = msg[h]
    for k in range(1, 2 * nb):
        total = total + recv[k]
    hv_out[...] = (total[:, :half] * scale).reshape(half)
    num_all = jnp.sum(jnp.where(spot == wide - 2, total, 0.0), axis=1, keepdims=True)
    den_all = jnp.sum(jnp.where(spot == wide - 1, total, 0.0), axis=1, keepdims=True)
    ex_out[...] = num_all / den_all
    v_copy.wait()


def flush(value, hands, value_out, hands_out, sem):
    pairs = ((value, value_out), (hands, hands_out))
    copies = [pltpu.make_async_copy(a, b, sem.at[k]) for k, (a, b) in enumerate(pairs)]
    for copy in copies:
        copy.start()
    for copy in copies:
        copy.wait()


def solution(mesh):
    nb = mesh.shape["board"]

    def local(opp_reach, hand_rank, hand_cards, pot, bet_frac, trav_reach):
        boards, half = opp_reach.shape
        hands = hand_rank.shape[1]
        own = boards // 2
        hp = up(hands, LANES)
        wide = up(half + 2, LANES)
        rows = up(PAIRS, 4) * 32
        tall = (2 * (PAIRS // 4) + 1) * LANES
        vm = pltpu.VMEM
        dma = pltpu.SemaphoreType.DMA
        value, hand_values, ratio = pl.pallas_call(
            functools.partial(kernel, nb),
            out_shape=(vm((boards, half), F32), vm((half,), F32), vm((1, 1), F32)),
            in_specs=[pl.BlockSpec(memory_space=pl.ANY)] * 6,
            scratch_shapes=[
                vm((2, hands), I32),
                vm((own, hands), I32),
                vm((own, half), BF16),
                vm((own, half), BF16),
                vm((own, hp), BF16),
                vm((own, hp), BF16),
                vm((own, hp), BF16),
                vm((half,), F32),
                vm((half,), F32),
                vm((1, boards), F32),
                vm((1, boards), F32),
                vm((2, hp), I32),
                vm((own, hp), I32),
                vm((own, hp), F32),
                vm((1, hp), F32),
                vm((2 * own, LANES), F32),
                vm((64, LANES), I32),
                vm((6, hp), I32),
                vm((16, hp), I32),
                vm((2, rows, LANES), I32),
                vm((tall, LANES), F32),
                vm((tall, LANES), F32),
                vm((tall, LANES), F32),
                vm((tall // BATCH, LANES), F32),
                vm((tall, LANES), F32),
                vm((2, LANES, LANES), F32),
                vm((2, rows, LANES), F32),
                vm((own * DIGIT, LANES), F32),
                vm((own, hp), F32),
                vm((own, hp), F32),
                vm((own, hp), F32),
                vm((own, up(TOPS, 16), hp), BF16),
                vm((own, hp), I32),
                vm((own, hp), I32),
                vm((own, LANES), F32),
                vm((own, LANES), F32),
                vm((own, hp), F32),
                vm((own, hp), F32),
                vm((own, hp), F32),
                vm((own, hp), F32),
                vm((2, hp), F32),
                vm((own, half), F32),
                vm((2, 1, wide), F32),
                vm((2 * nb, 1, wide), F32),
                dma((7,)),
                dma((2,)),
                dma((2,)),
                dma((2,)),
                dma,
                dma,
            ],
            compiler_params=pltpu.CompilerParams(collective_id=0, has_side_effects=True),
            name="main",
        )(opp_reach, hand_rank, hand_cards.T, pot[None, :], bet_frac[None, :], trav_reach)
        spot = pl.BlockSpec(memory_space=pl.ANY)
        value, hand_values = pl.pallas_call(
            flush,
            out_shape=tuple(jax.ShapeDtypeStruct(x.shape, x.dtype) for x in (value, hand_values)),
            in_specs=[spot] * 2,
            out_specs=[spot] * 2,
            scratch_shapes=[dma((2,))],
            name="flush",
        )(*(pltpu.with_memory_space_constraint(x, pltpu.VMEM) for x in (value, hand_values)))
        return value, hand_values, ratio[0, 0]

    placed = (P("board", "hand"), P("board", None), P(), P("board"), P("board"), P("hand"))
    return jax.shard_map(
        local,
        mesh=mesh,
        in_specs=placed,
        out_specs=(P("board", "hand"), P("hand"), P()),
        check_vma=False,
    )
```
